512 devices in a mesh: grp: 2 (over y), row: 32 (over z), col: 4 (over x), sub: 2 (over core).
Axes of the slice: x: 4, y: 2, z: 32, core: 2. Of those that a mesh axis runs over, the one named last changes fastest.
The devices are a block of a 4x8x32 slice.
Arguments:
- pair: bfloat16 [768, 384, 128], P(('grp', 'row'), 'col'), parts along dimension 0, may hold values from -6 to 6
- length: int32 [2], P('grp'), parts along dimension 0, may hold values from 192 to 384
- chain: int32 [768], P('grp'), parts along dimension 0, may hold values from 0 to 3, never falling along the last dimension, each value on 1 to 192 neighbouring positions
- att_proj: bfloat16 [128, 4, 128], P(None, None, 'sub'), may hold values from -0.5 to 0.5
- att_bias: bfloat16 [128, 4], P(None, 'sub')
- chain_bias: float32 [4], P('sub'), may hold values from -2 to 2
- att_out: bfloat16 [128, 128], P('sub'), may hold values from -0.5 to 0.5
- mult_in: bfloat16 [128, 512], replicated, may hold values from -0.5 to 0.5
- mult_gate: bfloat16 [128, 128], replicated, may hold values from -0.5 to 0.5
- mult_out: bfloat16 [128, 128], replicated, may hold values from -0.5 to 0.5
- trans_up: bfloat16 [128, 512], replicated, may hold values from -0.5 to 0.5
- trans_down: bfloat16 [512, 128], replicated, may hold values from -0.25 to 0.25
Outputs:
- pair_out: bfloat16 [768, 384, 128], P(('grp', 'row'), ('col', 'sub')), parts along dimension 0
The draws below stay inside these ranges and needn't reach their ends.
There are 2 independent parts, one for each index of `grp`. The reference program is written for one: setup_inputs(seed, part) draws one part's arguments, and reference() takes and returns one part's arrays. A program takes and returns all parts, laid end to end along the dimension named above; an argument that names none is the same for every part. Nothing has to cross between parts.
Inputs may be any that keep to these rules, and one draw needn't show every extreme that they name: chain numbers never fall along the residues; each chain has 1 to 192 residues.
All inputs are finite; a program needn't handle non-finite values.
Results may differ from the reference program's by a relative error of at most 0.012.
The reference program's roundings to bfloat16 on the way (of `normed`, `weights`, `attended`, `mixed` and `hidden`) count: a program that leaves them out, or rounds other values in their place, can miss the bound.
Values may be sent and summed in bfloat16 or wider, within the bound.
A program may use at most 64 MiB of HBM per device.

```python
import math
import jax
import jax.numpy as jnp
import numpy as np
from jax import lax

PAIR = 128
HEADS = 4
HEAD_DIM = 32
MULT = 128
TRANS = 512
RES = 384
N_COL = 4
N_SUB = 2


def draw_att_bias(key, part):
    first_key = jax.random.fold_in(key, 11)
    weights = jnp.clip(jax.random.normal(first_key, (PAIR, HEADS), jnp.float32), -6.0, 6.0) * PAIR ** (-0.5)
    return weights.astype(jnp.bfloat16)


def levels(stream_key, dims, pieces, low, high):
    def one(dim, parts):
        steps = jax.random.uniform(jax.random.fold_in(jax.random.fold_in(stream_key, 6), dim), (parts,), jnp.float32, low / len(pieces), high / len(pieces))
        return jnp.repeat(jnp.exp(steps), dims[dim] // parts).reshape((-1,) + (1,) * (len(dims) - dim - 1))

    level = one(*pieces[0])
    for cut in pieces[1:]:
        level = level * one(*cut)
    return level


def split_up(number_of, total, limit, slope):
    portions = [(1 << 20) // math.isqrt(rank ** slope) + 1 for rank in range(2, number_of + 1)]
    surplus, given = total - limit - (number_of - 1), [1] * (number_of - 1)
    while surplus > 0:
        movable = [i for i in range(number_of - 1) if given[i] < limit]
        mass, remaining = sum([portions[i] for i in movable]), surplus
        for i in movable:
            addition = min(limit - given[i], max(1, remaining * portions[i] // mass), surplus)
            given[i] = given[i] + addition
            surplus = surplus - addition
    return np.array([limit] + given)


def uneven(rng, amount, total, limit, lean):
    if amount == 2:
        one = jax.random.randint(rng, (), max(1, total - limit), min(limit, total - 1) + 1)
        return jnp.stack([one, total - one])
    lengths = jnp.asarray(split_up(amount, total, limit, lean), jnp.int32)
    couples = (amount - 1) // 2
    source_of, receiver = lengths[1:1 + 2 * couples:2], lengths[2:2 + 2 * couples:2]
    margin = jnp.minimum(source_of - 1, limit - receiver)
    moved = jax.random.randint(jax.random.fold_in(rng, 1), (couples,), 0, 1 << 20) % (margin + 1)
    lengths = lengths.at[1:1 + 2 * couples:2].set(source_of - moved).at[2:2 + 2 * couples:2].set(receiver + moved)
    return lengths[jax.random.permutation(jax.random.fold_in(rng, 2), amount)]


def bell_draw(own_key, extent, scale, limit, shards=(), held_as=jnp.bfloat16):
    loudness = levels(own_key, extent, shards, -0.22, 0.18) if shards else 1.0
    drawn = jax.random.normal(own_key, extent, jnp.float32) * scale * loudness
    return jnp.minimum(jnp.maximum(drawn, -limit), limit).astype(held_as)


def setup_inputs(seed: int = 0, part: int = 0) -> dict:
    key_list = jax.random.split(jax.random.key(seed), 13)
    part_splits = jax.random.split(jax.random.fold_in(key_list[12], part), 13)
    return {
        "pair": bell_draw(part_splits[0], (RES, RES, PAIR), 1.0, 6.0, ((0, 32), (1, 4))),
        "length": jax.random.randint(part_splits[1], (1,), RES // 2, RES + 1).astype(jnp.int32),
        "chain": jnp.searchsorted(jnp.cumsum(uneven(part_splits[2], 4, RES, RES // 2, 1)), jnp.arange(RES), side="right").astype(jnp.int32),
        "att_proj": bell_draw(key_list[3], (PAIR, 4, HEADS * HEAD_DIM), PAIR ** -0.5, 0.5, ((2, 2),)),
        "att_bias": draw_att_bias(jax.random.fold_in(key_list[12], 71), part),
        "chain_bias": jnp.clip(jax.random.uniform(key_list[5], (HEADS,), jnp.float32, -2.0, 2.0) * levels(key_list[5], (HEADS,), ((0, 2),), -0.4, 0.0), -2.0, 2.0),
        "att_out": bell_draw(key_list[6], (HEADS * HEAD_DIM, PAIR), (HEADS * HEAD_DIM) ** -0.5, 0.5, ((0, 2),)),
        "mult_in": bell_draw(key_list[7], (PAIR, 4 * MULT), PAIR ** -0.5, 0.5),
        "mult_gate": bell_draw(key_list[8], (PAIR, PAIR), PAIR ** -0.5, 0.5),
        "mult_out": bell_draw(key_list[9], (MULT, PAIR), MULT ** -0.5, 0.5),
        "trans_up": bell_draw(key_list[10], (PAIR, TRANS), PAIR ** -0.5, 0.5),
        "trans_down": bell_draw(key_list[11], (TRANS, PAIR), TRANS ** -0.5, 0.25),
    }


def norm(value):
    mean = lax.optimization_barrier(jnp.mean(value, axis=-1, keepdims=True))
    centred = value - mean
    variance = lax.optimization_barrier(jnp.mean(centred * centred, axis=-1, keepdims=True))
    return centred * lax.rsqrt(variance + 1e-05)

def reference(pair, length, chain, att_proj, att_bias, chain_bias, att_out, mult_in, mult_gate, mult_out, trans_up, trans_down):
    width = PAIR
    spread = HEADS * HEAD_DIM
    valid = (jnp.arange(RES) < length[0]).astype(jnp.float32)
    normed = norm(pair.astype(jnp.float32)).astype(jnp.bfloat16)
    flat = normed.reshape(RES * RES, width)
    projected = jnp.dot(flat, att_proj.reshape(width, 4 * spread), preferred_element_type=jnp.float32).reshape(RES, RES, 4, spread)
    query = (projected[:, :, 0] * HEAD_DIM ** (-0.5)).astype(jnp.bfloat16).reshape(RES // 2, 2, RES, HEADS, HEAD_DIM)
    keys = projected[:, :, 1].astype(jnp.bfloat16).reshape(RES // 2, 2, RES, HEADS, HEAD_DIM)
    values = projected[:, :, 2].astype(jnp.bfloat16).reshape(RES // 2, 2, RES, HEADS, HEAD_DIM)
    gating = jax.nn.sigmoid(projected[:, :, 3])
    bias = jnp.dot(flat, att_bias, preferred_element_type=jnp.float32).reshape(RES, RES, HEADS).transpose(2, 0, 1)
    same = (chain[:, None] == chain[None, :]).astype(jnp.float32)
    bias = bias + chain_bias[:, None, None] * same[None] + (valid[None, None, :] - 1.0) * 1000000000.0

    def attend(block):
        block_query, block_keys, block_values = block
        scores = jnp.einsum('ajhd,akhd->ahjk', block_query.astype(jnp.float32), block_keys.astype(jnp.float32)) + bias[None]
        weights = jax.nn.softmax(scores, axis=-1).astype(jnp.bfloat16)
        return jnp.einsum('ahjk,akhd->ajhd', weights.astype(jnp.float32), block_values.astype(jnp.float32))
    attended = lax.map(attend, (query, keys, values)).reshape(RES, RES, spread)
    attended = (attended * gating).astype(jnp.bfloat16)
    update = jnp.dot(attended.reshape(RES * RES, spread), att_out, preferred_element_type=jnp.float32)
    first = pair.astype(jnp.float32) + update.reshape(RES, RES, width)
    mixed = norm(first).astype(jnp.bfloat16).reshape(RES * RES, width)
    mult_width = MULT
    quad = jnp.dot(mixed, mult_in, preferred_element_type=jnp.float32).reshape(RES, RES, 4, mult_width)
    outer = valid[:, None, None] * valid[None, :, None]
    left = (outer * jax.nn.sigmoid(quad[:, :, 1]) * quad[:, :, 0]).astype(jnp.bfloat16)
    right = (outer * jax.nn.sigmoid(quad[:, :, 3]) * quad[:, :, 2]).astype(jnp.bfloat16)
    blocks = N_COL * N_SUB
    block_width = RES // blocks

    def accumulate(index, total):
        start = (index * block_width).astype(jnp.int32)
        left_block = lax.dynamic_slice_in_dim(left, start, block_width, 1).astype(jnp.float32)
        right_block = lax.dynamic_slice_in_dim(right, start, block_width, 1).astype(jnp.float32)
        partial_value = jnp.einsum('ikc,jkc->ijc', left_block, right_block).astype(jnp.bfloat16)
        partial_value = lax.optimization_barrier(partial_value)
        return total + partial_value.astype(jnp.float32)
    tri = lax.fori_loop(jnp.int32(0), jnp.int32(blocks), accumulate, jnp.zeros((RES, RES, mult_width), jnp.float32))
    gate_out = jax.nn.sigmoid(jnp.dot(mixed, mult_gate, preferred_element_type=jnp.float32))
    tri_normed = norm(tri).astype(jnp.bfloat16).reshape(RES * RES, mult_width)
    second = first + (gate_out * jnp.dot(tri_normed, mult_out, preferred_element_type=jnp.float32)).reshape(RES, RES, width)
    last_normed = norm(second).astype(jnp.bfloat16).reshape(RES * RES, width)
    hidden = jax.nn.relu(jnp.dot(last_normed, trans_up, preferred_element_type=jnp.float32)).astype(jnp.bfloat16)
    result = second + jnp.dot(hidden, trans_down, preferred_element_type=jnp.float32).reshape(RES, RES, width)
    return result.astype(jnp.bfloat16)
```

```python
import functools

import jax
import jax.numpy as jnp
from jax import lax
from jax.experimental import pallas as pl
from jax.experimental.pallas import tpu as pltpu
from jax.sharding import PartitionSpec as P

MESH = pl.DeviceIdType.MESH
CHUNKS = 4


def sent_together(arrays, axis, dim, along):
    ends, at = ([], 0)
    for a in arrays[:-1]:
        at += a.shape[along]
        ends.append(at)
    both = jnp.concatenate(arrays, axis=along)
    return tuple(jnp.split(lax.all_gather(both, axis, axis=dim, tiled=True), ends, axis=along))


def joined_along(blocks, dim):
    shape = list(blocks.shape[1:])
    shape[dim] *= blocks.shape[0]
    return jnp.moveaxis(blocks, 0, dim).reshape(shape)


def copy_for_each(shard, axis):
    devices = lax.axis_size(axis)
    return lax.all_to_all(
        jnp.broadcast_to(shard[None], (devices, *shard.shape)), axis, 0, 0, tiled=True
    )


def collect(shard, axis, dim):
    return joined_along(copy_for_each(shard, axis), dim)


def cut_along(shard, dim, devices):
    before, after = (shard.shape[:dim], shard.shape[dim + 1 :])
    return jnp.moveaxis(shard.reshape(*before, devices, -1, *after), dim, 0)


def sum_at_owner(shard, axis, dim):
    devices = lax.axis_size(axis)
    blocks = lax.all_to_all(cut_along(shard, dim, devices), axis, 0, 0, tiled=True)
    return jnp.sum(blocks.astype(jnp.float32), axis=0)


def norm(value):
    mean = jnp.mean(value, axis=-1, keepdims=True)
    centred = value - mean
    variance = jnp.mean(centred * centred, axis=-1, keepdims=True)
    return centred * lax.rsqrt(variance + 1e-05)


def tail_kernel(
    n_row,
    n_col,
    n_sub,
    length_ref,
    first_ref,
    mult_in_ref,
    mult_gate_ref,
    mult_out_ref,
    trans_up_ref,
    trans_down_ref,
    out_ref,
    gathered,
    left,
    stage_f32,
    stage,
    parts,
    tri,
    gate,
    ring_send,
    ring_recv,
    part_send,
    part_recv,
):
    rows, half, width = first_ref.shape
    piece = rows // CHUNKS
    z = lax.axis_index("row")
    x = lax.axis_index("col")
    core = lax.axis_index("sub")
    owners = n_col * n_sub
    me = x * n_sub + core
    per_owner = n_row // owners
    far = n_row // 2
    up = lax.rem(z + 1, n_row)
    down = lax.rem(z + n_row - 1, n_row)

    barrier = pltpu.get_barrier_semaphore()
    for other in (up, down):
        pl.semaphore_signal(barrier, inc=1, device_id={"row": other}, device_id_type=MESH)
    for step in range(1, owners):
        other = lax.rem(me + step, owners)
        pl.semaphore_signal(
            barrier,
            inc=1,
            device_id={"col": lax.div(other, n_sub), "sub": lax.rem(other, n_sub)},
            device_id_type=MESH,
        )

    first = first_ref[...].reshape(rows * half, width)
    mixed = norm(first).astype(jnp.bfloat16)
    quad = jnp.dot(mixed, mult_in_ref[...], preferred_element_type=jnp.float32)
    shape = (rows, half, width)
    here_row = z * rows + lax.broadcasted_iota(jnp.int32, shape, 0)
    here_col = (x * n_sub + core) * half + lax.broadcasted_iota(jnp.int32, shape, 1)
    length = length_ref[0]
    valid = ((here_row < length) & (here_col < length)).astype(jnp.float32)
    a, b, c, d = [quad[:, k * width : (k + 1) * width].reshape(shape) for k in range(4)]
    left[...] = (valid * jax.nn.sigmoid(b) * a).astype(jnp.bfloat16).astype(jnp.float32)
    gathered[z] = (valid * jax.nn.sigmoid(d) * c).astype(jnp.bfloat16)
    gate[...] = jax.nn.sigmoid(
        jnp.dot(mixed, mult_gate_ref[...], preferred_element_type=jnp.float32)
    )
    pl.semaphore_wait(barrier, 2 + owners - 1)

    def source(way, step):
        return lax.rem(z + (n_row - step if way == 0 else step), n_row)

    def ring_copy(way, step, chunk, arrives):
        block = gathered.at[source(way, step), pl.ds(chunk * piece, piece)]
        return pltpu.make_async_remote_copy(
            src_ref=block,
            dst_ref=block,
            send_sem=ring_send.at[way, lax.rem(step, 2), chunk],
            recv_sem=ring_recv.at[way, step - 1 if arrives else step, chunk],
            device_id={"row": up if way == 0 else down},
            device_id_type=MESH,
        )

    def hop(way, step, chunk):
        return ring_copy(way, step, chunk, False)

    def arrival(way, step, chunk):
        return ring_copy(way, step, chunk, True)

    def multiply(owner, chunk, lane):
        for jj in range(piece):
            j = chunk * piece + jj
            right = gathered[owner, j].astype(jnp.float32)
            for i in range(rows):
                stage_f32[lane, pl.ds(i * rows + j, 1)] = jnp.sum(
                    left[i] * right, axis=0, keepdims=True
                )

    def part_copy(block):
        dest = lax.div(block, per_owner)
        slot = lax.rem(block, per_owner)
        return pltpu.make_async_remote_copy(
            src_ref=stage.at[block],
            dst_ref=parts.at[me, slot],
            send_sem=part_send.at[block],
            recv_sem=part_recv.at[me, slot],
            device_id={"col": lax.div(dest, n_sub), "sub": lax.rem(dest, n_sub)},
            device_id_type=MESH,
        )

    def give(block, lane):
        slot = lax.rem(block, per_owner)
        mine = lax.div(block, per_owner) == me
        stage[block] = stage_f32[lane].astype(jnp.bfloat16)

        @pl.when(mine)
        def _():
            pltpu.make_async_copy(
                stage.at[block], parts.at[me, slot], part_recv.at[me, slot]
            ).start()

        @pl.when(jnp.logical_not(mine))
        def _():
            part_copy(block).start()

    for chunk in range(CHUNKS):
        for way in range(2):
            hop(way, 0, chunk).start()

    def own(chunk, carry):
        multiply(z, chunk, 0)
        return carry

    lax.fori_loop(0, CHUNKS, own, 0)
    give(z, 0)

    def visit(n, carry):
        step = lax.div(n, CHUNKS) + 1
        chunk = lax.rem(n, CHUNKS)
        for way in range(2):
            arrival(way, step, chunk).wait_recv()
            last = chunk < CHUNKS // 2 if way == 0 else chunk >= CHUNKS // 2

            @pl.when(step >= 2)
            def _():
                hop(way, step, chunk).wait_send()

            @pl.when(jnp.logical_or(step < far - 1, last))
            def _():
                hop(way, step, chunk).start()

        for way in range(2):
            multiply(source(way, step), chunk, way)

        @pl.when(chunk == CHUNKS - 1)
        def _():
            for way in range(2):
                give(source(way, step), way)

        return carry

    lax.fori_loop(0, (far - 1) * CHUNKS, visit, 0)

    for chunk in range(CHUNKS):
        arrival(0 if chunk < CHUNKS // 2 else 1, far, chunk).wait_recv()
        multiply(source(0, far), chunk, 0)
    give(source(0, far), 0)

    for way in range(2):
        for chunk in range(CHUNKS):
            hop(way, far - 2, chunk).wait_send()
            if (chunk < CHUNKS // 2) == (way == 0):
                hop(way, far - 1, chunk).wait_send()

    for block in range(n_row):

        @pl.when(block // per_owner != me)
        def _():
            part_copy(block).wait_send()

    for slot in range(per_owner):
        total = None
        for giver in range(owners):
            pltpu.make_async_copy(
                stage.at[0], parts.at[giver, slot], part_recv.at[giver, slot]
            ).wait()
            part = parts[giver, slot].astype(jnp.float32)
            total = part if total is None else total + part
        for i in range(rows):
            tri[i, slot * rows : (slot + 1) * rows] = total[i * rows : (i + 1) * rows]

    tri_normed = norm(tri[...].reshape(rows * half, width)).astype(jnp.bfloat16)
    second = first_ref[...].reshape(rows * half, width) + gate[...] * jnp.dot(
        tri_normed, mult_out_ref[...], preferred_element_type=jnp.float32
    )
    last_normed = norm(second).astype(jnp.bfloat16)
    hidden = jax.nn.relu(
        jnp.dot(last_normed, trans_up_ref[...], preferred_element_type=jnp.float32)
    ).astype(jnp.bfloat16)
    result = second + jnp.dot(hidden, trans_down_ref[...], preferred_element_type=jnp.float32)
    out_ref[...] = result.astype(jnp.bfloat16).reshape(rows, half, width)


def tail(first, length, mult_in, mult_gate, mult_out, trans_up, trans_down):
    rows, half, width = first.shape
    n_row, n_col, n_sub = (lax.axis_size(a) for a in ("row", "col", "sub"))
    owners = n_col * n_sub
    vmem = pl.BlockSpec(memory_space=pltpu.VMEM)
    return pl.pallas_call(
        functools.partial(tail_kernel, n_row, n_col, n_sub),
        out_shape=jax.ShapeDtypeStruct(first.shape, jnp.bfloat16),
        in_specs=[pl.BlockSpec(memory_space=pltpu.SMEM)] + [vmem] * 6,
        out_specs=vmem,
        scratch_shapes=[
            pltpu.VMEM((n_row, rows, half, width), jnp.bfloat16),
            pltpu.VMEM((rows, half, width), jnp.float32),
            pltpu.VMEM((2, rows * rows, width), jnp.float32),
            pltpu.VMEM((n_row, rows * rows, width), jnp.bfloat16),
            pltpu.VMEM((owners, n_row // owners, rows * rows, width), jnp.bfloat16),
            pltpu.VMEM((rows, half, width), jnp.float32),
            pltpu.VMEM((rows * half, width), jnp.float32),
            pltpu.SemaphoreType.DMA((2, 2, CHUNKS)),
            pltpu.SemaphoreType.DMA((2, n_row // 2, CHUNKS)),
            pltpu.SemaphoreType.DMA((n_row,)),
            pltpu.SemaphoreType.DMA((owners, n_row // owners)),
        ],
        compiler_params=pltpu.CompilerParams(collective_id=0, has_side_effects=True),
    )(length, first, mult_in, mult_gate, mult_out, trans_up, trans_down)


def local(
    pair,
    length,
    chain,
    att_proj,
    att_bias,
    chain_bias,
    att_out,
    mult_in,
    mult_gate,
    mult_out,
    trans_up,
    trans_down,
):
    rows, cols, width = pair.shape
    row_count = lax.axis_size("row")
    sub_count = lax.axis_size("sub")
    col_index = lax.axis_index("col")
    sub_index = lax.axis_index("sub")
    total = rows * row_count
    half = cols // sub_count
    heads_here = att_bias.shape[1]
    spread = att_out.shape[0]
    head_dim = spread // heads_here
    valid = (jnp.arange(total) < length[0]).astype(jnp.float32)
    normed = norm(pair.astype(jnp.float32)).astype(jnp.bfloat16)
    flat = normed.reshape(rows * cols, width)
    projected = jnp.dot(
        flat, att_proj.reshape(width, 4 * spread), preferred_element_type=jnp.float32
    ).reshape(rows, cols, 4, spread)
    query = (projected[:, :, 0] * head_dim ** (-0.5)).astype(jnp.bfloat16)
    keys = projected[:, :, 1].astype(jnp.bfloat16)
    values = projected[:, :, 2].astype(jnp.bfloat16)
    gating = jax.nn.sigmoid(projected[:, :, 3])
    bias_local = (
        jnp.dot(flat, att_bias, preferred_element_type=jnp.float32)
        .reshape(rows, cols, heads_here)
        .transpose(2, 0, 1)
    )
    keys_all, values_all = sent_together((keys, values), "col", 1, 0)
    column_bias = collect(bias_local, "row", 1)
    bias_here = lax.all_to_all(column_bias, "col", split_axis=1, concat_axis=2, tiled=True)
    chain_here = lax.dynamic_slice_in_dim(chain, col_index * cols, cols, 0)
    same = (chain_here[:, None] == chain[None, :]).astype(jnp.float32)
    bias_here = (
        bias_here
        + chain_bias[:, None, None] * same[None]
        + (valid[None, None, :] - 1.0) * 1000000000.0
    )

    def attend(block):
        block_query, block_keys, block_values = block
        scores = (
            jnp.einsum(
                "ajhd,akhd->ahjk", block_query, block_keys, preferred_element_type=jnp.float32
            )
            + bias_here[None]
        )
        weights = jax.nn.softmax(scores, axis=-1).astype(jnp.bfloat16)
        return jnp.einsum(
            "ahjk,akhd->ajhd", weights, block_values, preferred_element_type=jnp.float32
        )

    attended = lax.map(
        attend,
        (
            query.reshape(rows // 2, 2, cols, heads_here, head_dim),
            keys_all.reshape(rows // 2, 2, total, heads_here, head_dim),
            values_all.reshape(rows // 2, 2, total, heads_here, head_dim),
        ),
    )
    attended = (attended.reshape(rows, cols, spread) * gating).astype(jnp.bfloat16)
    update = jnp.dot(
        attended.reshape(rows * cols, spread), att_out, preferred_element_type=jnp.float32
    ).reshape(rows, cols, width)
    update_half = sum_at_owner(update.astype(jnp.bfloat16), "sub", 1)
    pair_half = lax.dynamic_slice_in_dim(pair, sub_index * half, half, 1).astype(jnp.float32)
    first = pair_half + update_half
    return tail(first, length, mult_in, mult_gate, mult_out, trans_up, trans_down)


def solution(mesh):
    placed = (
        P(("grp", "row"), "col", None),
        P("grp"),
        P("grp"),
        P(None, None, "sub"),
        P(None, "sub"),
        P("sub"),
        P("sub", None),
        P(),
        P(),
        P(),
        P(),
        P(),
    )
    return jax.shard_map(
        local,
        mesh=mesh,
        in_specs=placed,
        out_specs=P(("grp", "row"), ("col", "sub"), None),
        check_vma=False,
    )
```

```python
import functools

import jax
import jax.numpy as jnp
from jax import lax
from jax.experimental import pallas as pl
from jax.experimental.pallas import tpu as pltpu
from jax.sharding import PartitionSpec as P

MESH = pl.DeviceIdType.MESH
CHUNKS = 4
STRIDE = 4
LOCAL = (-1, 1, 2)


def norm(value):
    mean = jnp.mean(value, axis=-1, keepdims=True)
    centred = value - mean
    variance = jnp.mean(centred * centred, axis=-1, keepdims=True)
    return centred * lax.rsqrt(variance + 1e-05)


def pair_kernel(
    n_row,
    n_col,
    n_sub,
    length_ref,
    chain_ref,
    chain_bias_ref,
    pair_ref,
    chain_cols_ref,
    bias_w_ref,
    att_w_ref,
    att_out_ref,
    mult_in_ref,
    mult_gate_ref,
    mult_out_ref,
    trans_up_ref,
    trans_down_ref,
    out_ref,
    normed,
    kept,
    queries,
    att_gate,
    scores,
    bias,
    pieces,
    bias_in,
    other_w,
    both_out,
    attended,
    first_ref,
    gathered,
    left,
    stage_f32,
    stage,
    parts,
    tri,
    gate,
    x_send,
    x_recv,
    weight_send,
    weight_recv,
    chain_send,
    chain_recv,
    bias_send,
    bias_recv,
    ring_send,
    ring_recv,
    part_send,
    part_recv,
):
    rows, cols, width = pair_ref.shape
    half = cols // n_sub
    total = rows * n_row
    piece = rows // CHUNKS
    block_rows = rows // 2
    heads_here = pieces.shape[1] // rows
    heads = heads_here * n_sub
    head_dim = width // heads
    z = lax.axis_index("row")
    x = lax.axis_index("col")
    core = lax.axis_index("sub")
    owners = n_col * n_sub
    me = x * n_sub + core
    per_owner = n_row // owners
    far = n_row // 2
    up = lax.rem(z + 1, n_row)
    down = lax.rem(z + n_row - 1, n_row)
    length = length_ref[0]

    def row_at(offset):
        return lax.rem(z + (offset + n_row), n_row)

    barrier = pltpu.get_barrier_semaphore()
    near = (1, -1, 2, -2, STRIDE, -STRIDE)
    for offset in near:
        pl.semaphore_signal(
            barrier, inc=1, device_id={"row": row_at(offset)}, device_id_type=MESH
        )
    for step in range(1, owners):
        other = lax.rem(me + step, owners)
        pl.semaphore_signal(
            barrier,
            inc=1,
            device_id={"col": lax.div(other, n_sub), "sub": lax.rem(other, n_sub)},
            device_id_type=MESH,
        )

    normed[x] = norm(pair_ref[...].astype(jnp.float32)).astype(jnp.bfloat16)
    both_out[core] = att_out_ref[...]

    lane = lax.broadcasted_iota(jnp.int32, (8, width), 1)
    line = lax.broadcasted_iota(jnp.int32, (8, width), 0)
    chain_bias = jnp.zeros((8, width), jnp.float32)
    for h in range(heads_here):
        chain_bias = jnp.where(line == h, chain_bias_ref[h], chain_bias)
    key_valid = ((x * cols + lane) < length).astype(jnp.float32)
    padding = jnp.zeros((width - cols, width), jnp.bfloat16)
    for i in range(rows):
        keys_i = jnp.concatenate([normed[x, i], padding], axis=0)
        term = lax.dot_general(
            bias_w_ref[...], keys_i, (((1,), (1,)), ((), ())), preferred_element_type=jnp.float32
        )
        same = (chain_cols_ref[...] == chain_ref[z * rows + i]).astype(jnp.float32)
        term = term + chain_bias * same + (key_valid - 1.0) * 1000000000.0
        term = pltpu.roll(term, lax.rem(x * cols, width), 1)
        for h in range(heads_here):
            pieces[z, h * rows + i : h * rows + i + 1] = term[h : h + 1]

    pl.semaphore_wait(barrier, len(near) + owners - 1)

    def weight_copy(k):
        source, target = [(att_w_ref, other_w), (both_out.at[core], both_out.at[core])][k]
        return pltpu.make_async_remote_copy(
            src_ref=source,
            dst_ref=target,
            send_sem=weight_send.at[k],
            recv_sem=weight_recv.at[k],
            device_id={"sub": 1 - core},
            device_id_type=MESH,
        )

    def x_copy(way, step, chunk, arrives):
        distance = step + 1 if arrives else step
        source = lax.rem(x + (n_col - distance if way == 0 else distance), n_col)
        block = normed.at[source, pl.ds(chunk * block_rows, block_rows)]
        return pltpu.make_async_remote_copy(
            src_ref=block,
            dst_ref=block,
            send_sem=x_send.at[way, step, chunk],
            recv_sem=x_recv.at[way, step, chunk],
            device_id={"col": lax.rem(x + (1 if way == 0 else n_col - 1), n_col)},
            device_id_type=MESH,
        )

    def bias_hop(stop, k, block, offset):
        return pltpu.make_async_remote_copy(
            src_ref=pieces.at[block],
            dst_ref=pieces.at[block],
            send_sem=chain_send.at[stop, k],
            recv_sem=chain_recv.at[block],
            device_id={"row": row_at(offset)},
            device_id_type=MESH,
        )

    def owner_copy(block, source, target, send_sem, recv_sem):
        dest = lax.div(block, per_owner)
        return pltpu.make_async_remote_copy(
            src_ref=source.at[block],
            dst_ref=target.at[me, lax.rem(block, per_owner)],
            send_sem=send_sem.at[block],
            recv_sem=recv_sem.at[me, lax.rem(block, per_owner)],
            device_id={"col": lax.div(dest, n_sub), "sub": lax.rem(dest, n_sub)},
            device_id_type=MESH,
        )

    def to_owner(block, source, target, send_sem, recv_sem):
        slot = lax.rem(block, per_owner)
        mine = lax.div(block, per_owner) == me

        @pl.when(mine)
        def _():
            pltpu.make_async_copy(
                source.at[block], target.at[me, slot], recv_sem.at[me, slot]
            ).start()

        @pl.when(jnp.logical_not(mine))
        def _():
            owner_copy(block, source, target, send_sem, recv_sem).start()

    bias_way = (pieces, bias_in, bias_send, bias_recv)
    part_way = (stage, parts, part_send, part_recv)
    ups = n_row // (2 * STRIDE)

    def hops_of(stop):
        if stop == 0:
            ahead = [(0, STRIDE), (len(LOCAL) + 1, -STRIDE)]
        elif stop < ups:
            ahead = [(0, STRIDE)]
        elif stop == ups or stop == 2 * ups - 1:
            ahead = []
        else:
            ahead = [(0, -STRIDE)]
        return ahead + [(1 + n, offset) for n, offset in enumerate(LOCAL)]

    def block_of(stop):
        return row_at(-STRIDE * stop if stop <= ups else STRIDE * (stop - ups))

    def pass_on(stop):
        block = block_of(stop)
        if stop > 0:
            bias_hop(stop, 0, block, 0).wait_recv()
        for k, offset in hops_of(stop):
            bias_hop(stop, k, block, offset).start()
        to_owner(block, *bias_way)

    def take_local(stop):
        for offset in LOCAL:
            block = lax.rem(block_of(stop) + (n_row - offset), n_row)
            bias_hop(stop, 0, block, 0).wait_recv()
            to_owner(block, *bias_way)

    def project(source, chunk):
        tile = normed[source, pl.ds(chunk * block_rows, block_rows)]
        made = jnp.dot(
            tile.reshape(block_rows * cols, width),
            w_all[:, width : 3 * width],
            preferred_element_type=jnp.float32,
        ).astype(jnp.bfloat16)
        kept[
            pl.ds(chunk * block_rows, block_rows), pl.ds(pl.multiple_of(source * cols, 32), cols)
        ] = made.reshape(block_rows, cols, 2 * width)

    def score(i, carry):
        scores[i] = lax.dot_general(
            queries[i],
            kept[i, :, :width],
            (((1,), (1,)), ((), ())),
            preferred_element_type=jnp.float32,
        )
        return carry

    pass_on(0)
    for k in range(2):
        weight_copy(k).start()
    for chunk in range(2):
        for way in range(2):
            x_copy(way, 0, chunk if way == 0 else 1 - chunk, False).start()

    for k in range(2):
        weight_copy(k).wait_recv()
    w_all = att_w_ref[...] + other_w[...]
    tile = normed[x, :, pl.ds(pl.multiple_of(core * half, 16), half)].reshape(rows * half, width)
    query = (
        jnp.dot(tile, w_all[:, :width], preferred_element_type=jnp.float32) * head_dim ** (-0.5)
    ).astype(jnp.bfloat16)
    head_of = lax.broadcasted_iota(jnp.int32, (rows * half, width), 1) // head_dim
    for h in range(heads):
        queries[:, h * half : (h + 1) * half] = jnp.where(
            head_of == h, query, jnp.zeros_like(query)
        ).reshape(rows, half, width)
    att_gate[...] = jax.nn.sigmoid(
        jnp.dot(tile, w_all[:, 3 * width :], preferred_element_type=jnp.float32)
    ).reshape(rows, half, width)
    for chunk in range(2):
        project(x, chunk)

    x_up = lax.rem(x + n_col - 1, n_col)
    x_down = lax.rem(x + 1, n_col)
    x_far = lax.rem(x + 2, n_col)

    def stage_of(step):
        if step <= ups:
            pass_on(step)
        if step < ups:
            pass_on(ups + step)
        take_local(step - 1)
        if 1 <= step - 1 < ups:
            take_local(ups + step - 1)

    stage_of(1)
    x_copy(0, 0, 0, True).wait_recv()
    x_copy(0, 1, 0, False).start()
    x_copy(1, 0, 1, True).wait_recv()
    x_copy(1, 1, 1, False).start()
    project(x_up, 0)
    project(x_down, 1)
    stage_of(2)
    x_copy(0, 0, 1, True).wait_recv()
    project(x_up, 1)
    x_copy(1, 0, 0, True).wait_recv()
    project(x_down, 0)
    stage_of(3)
    x_copy(0, 1, 0, True).wait_recv()
    project(x_far, 0)
    lax.fori_loop(0, block_rows, score, 0)
    stage_of(4)
    x_copy(1, 1, 1, True).wait_recv()
    project(x_far, 1)
    lax.fori_loop(block_rows, rows, score, 0)
    take_local(ups)

    for slot in range(per_owner):
        for giver in range(owners):
            pltpu.make_async_copy(
                pieces.at[0], bias_in.at[giver, slot], bias_recv.at[giver, slot]
            ).wait()
    lane = lax.broadcasted_iota(jnp.int32, (rows, width), 1)
    for slot in range(per_owner):
        for h in range(heads):
            giver, own_head = h // heads_here, h % heads_here
            held = [
                bias_in[k * n_sub + giver, slot, own_head * rows : (own_head + 1) * rows]
                for k in range(n_col)
            ]
            at = h * half + slot * rows
            for k in range(total // width):
                line = None
                for source in range(n_col):
                    begin = source * cols - k * width
                    if begin + cols <= 0 or begin >= width:
                        continue
                    line = held[source] if line is None else jnp.where(lane >= begin, held[source], line)
                bias[at : at + rows, k * width : (k + 1) * width] = line

    head_of = lax.broadcasted_iota(jnp.int32, (half, width), 1) // head_dim

    def attend(i, carry):
        logits = scores[i] + bias[...]
        weights = jnp.exp(logits - jnp.max(logits, axis=-1, keepdims=True))
        weights = weights * (1.0 / jnp.sum(weights, axis=-1, keepdims=True))
        mixed_values = jnp.dot(
            weights.astype(jnp.bfloat16), kept[i, :, width:], preferred_element_type=jnp.float32
        )
        taken = jnp.zeros((half, width), jnp.float32)
        for h in range(heads):
            taken = jnp.where(head_of == h, mixed_values[h * half : (h + 1) * half], taken)
        attended[i] = (taken * att_gate[i]).astype(jnp.bfloat16)
        return carry

    lax.fori_loop(0, rows, attend, 0, unroll=2)
    first_ref[...] = pair_ref[:, pl.ds(pl.multiple_of(core * half, 16), half)].astype(
        jnp.float32
    ) + jnp.dot(
        attended[...].reshape(rows * half, width),
        both_out[...].reshape(width, width),
        preferred_element_type=jnp.float32,
    ).reshape(rows, half, width)

    first = first_ref[...].reshape(rows * half, width)
    mixed = norm(first).astype(jnp.bfloat16)
    quad = jnp.dot(mixed, mult_in_ref[...], preferred_element_type=jnp.float32)
    shape = (rows, half, width)
    here_row = z * rows + lax.broadcasted_iota(jnp.int32, shape, 0)
    here_col = (x * n_sub + core) * half + lax.broadcasted_iota(jnp.int32, shape, 1)
    valid = ((here_row < length) & (here_col < length)).astype(jnp.float32)
    a, b, c, d = [quad[:, k * width : (k + 1) * width].reshape(shape) for k in range(4)]
    left[...] = (valid * jax.nn.sigmoid(b) * a).astype(jnp.bfloat16).astype(jnp.float32)
    gathered[z] = (valid * jax.nn.sigmoid(d) * c).astype(jnp.bfloat16)
    gate[...] = jax.nn.sigmoid(
        jnp.dot(mixed, mult_gate_ref[...], preferred_element_type=jnp.float32)
    )

    def source(way, step):
        return lax.rem(z + (n_row - step if way == 0 else step), n_row)

    def ring_copy(way, step, chunk, arrives):
        block = gathered.at[source(way, step), pl.ds(chunk * piece, piece)]
        return pltpu.make_async_remote_copy(
            src_ref=block,
            dst_ref=block,
            send_sem=ring_send.at[way, lax.rem(step, 2), chunk],
            recv_sem=ring_recv.at[way, step - 1 if arrives else step, chunk],
            device_id={"row": up if way == 0 else down},
            device_id_type=MESH,
        )

    def hop(way, step, chunk):
        return ring_copy(way, step, chunk, False)

    def arrival(way, step, chunk):
        return ring_copy(way, step, chunk, True)

    def multiply(owner, chunk, lane):
        for jj in range(piece):
            j = chunk * piece + jj
            right = gathered[owner, j].astype(jnp.float32)
            for i in range(rows):
                stage_f32[lane, pl.ds(i * rows + j, 1)] = jnp.sum(
                    left[i] * right, axis=0, keepdims=True
                )

    def give(block, lane):
        stage[block] = stage_f32[lane].astype(jnp.bfloat16)
        to_owner(block, *part_way)

    for chunk in range(CHUNKS):
        for way in range(2):
            hop(way, 0, chunk).start()

    def own(chunk, carry):
        multiply(z, chunk, 0)
        return carry

    lax.fori_loop(0, CHUNKS, own, 0)
    give(z, 0)

    def visit(n, carry):
        step = lax.div(n, CHUNKS) + 1
        chunk = lax.rem(n, CHUNKS)
        for way in range(2):
            arrival(way, step, chunk).wait_recv()
            last = chunk < CHUNKS // 2 if way == 0 else chunk >= CHUNKS // 2

            @pl.when(step >= 2)
            def _():
                hop(way, step, chunk).wait_send()

            @pl.when(jnp.logical_or(step < far - 1, last))
            def _():
                hop(way, step, chunk).start()

        for way in range(2):
            multiply(source(way, step), chunk, way)

        @pl.when(chunk == CHUNKS - 1)
        def _():
            for way in range(2):
                give(source(way, step), way)

        return carry

    lax.fori_loop(0, (far - 1) * CHUNKS, visit, 0)

    for chunk in range(CHUNKS):
        arrival(0 if chunk < CHUNKS // 2 else 1, far, chunk).wait_recv()
        multiply(source(0, far), chunk, 0)
    give(source(0, far), 0)

    for way in range(2):
        for chunk in range(CHUNKS):
            hop(way, far - 2, chunk).wait_send()
            if (chunk < CHUNKS // 2) == (way == 0):
                hop(way, far - 1, chunk).wait_send()

    for stop in range(2 * ups):
        for k, offset in hops_of(stop):
            bias_hop(stop, k, block_of(stop), offset).wait_send()
    for k in range(2):
        weight_copy(k).wait_send()
    for way in range(2):
        for chunk in range(2):
            x_copy(way, 0, chunk, False).wait_send()
        x_copy(way, 1, way, False).wait_send()

    def sent(block, carry):
        @pl.when(lax.div(block, per_owner) != me)
        def _():
            owner_copy(block, *bias_way).wait_send()
            owner_copy(block, *part_way).wait_send()

        return carry

    lax.fori_loop(0, n_row, sent, 0)

    for slot in range(per_owner):
        total_f32 = None
        for giver in range(owners):
            pltpu.make_async_copy(
                stage.at[0], parts.at[giver, slot], part_recv.at[giver, slot]
            ).wait()
            part = parts[giver, slot].astype(jnp.float32)
            total_f32 = part if total_f32 is None else total_f32 + part
        for i in range(rows):
            tri[i, slot * rows : (slot + 1) * rows] = total_f32[i * rows : (i + 1) * rows]

    tri_normed = norm(tri[...].reshape(rows * half, width)).astype(jnp.bfloat16)
    second = first_ref[...].reshape(rows * half, width) + gate[...] * jnp.dot(
        tri_normed, mult_out_ref[...], preferred_element_type=jnp.float32
    )
    last_normed = norm(second).astype(jnp.bfloat16)
    hidden = jax.nn.relu(
        jnp.dot(last_normed, trans_up_ref[...], preferred_element_type=jnp.float32)
    ).astype(jnp.bfloat16)
    result = second + jnp.dot(hidden, trans_down_ref[...], preferred_element_type=jnp.float32)
    out_ref[...] = result.astype(jnp.bfloat16).reshape(rows, half, width)


def local(
    pair,
    length,
    chain,
    att_proj,
    att_bias,
    chain_bias,
    att_out,
    mult_in,
    mult_gate,
    mult_out,
    trans_up,
    trans_down,
):
    rows, cols, width = pair.shape
    n_row, n_col, n_sub = (lax.axis_size(a) for a in ("row", "col", "sub"))
    owners = n_col * n_sub
    per_owner = n_row // owners
    half = cols // n_sub
    total = rows * n_row
    heads_here = att_bias.shape[1]
    heads = heads_here * n_sub
    spread = att_out.shape[0]
    chain_cols = jnp.pad(
        lax.dynamic_slice_in_dim(chain, lax.axis_index("col") * cols, cols, 0), (0, width - cols)
    )[None]
    bias_w = jnp.pad(att_bias.T, ((0, 8 - heads_here), (0, 0)))
    att_w = lax.dynamic_update_slice_in_dim(
        jnp.zeros((width, 4, spread * n_sub), jnp.bfloat16),
        att_proj,
        lax.axis_index("sub") * spread,
        2,
    ).reshape(width, 4 * spread * n_sub)
    vmem = pl.BlockSpec(memory_space=pltpu.VMEM)
    smem = pl.BlockSpec(memory_space=pltpu.SMEM)
    dma = pltpu.SemaphoreType.DMA
    bf16, f32 = jnp.bfloat16, jnp.float32
    return pl.pallas_call(
        functools.partial(pair_kernel, n_row, n_col, n_sub),
        out_shape=jax.ShapeDtypeStruct((rows, half, width), bf16),
        in_specs=[smem] * 3 + [vmem] * 10,
        out_specs=vmem,
        scratch_shapes=[
            pltpu.VMEM((n_col, rows, cols, width), bf16),
            pltpu.VMEM((rows, total, 2 * width), bf16),
            pltpu.VMEM((rows, heads * half, width), bf16),
            pltpu.VMEM((rows, half, width), f32),
            pltpu.VMEM((rows, heads * half, total), f32),
            pltpu.VMEM((heads * half, total), f32),
            pltpu.VMEM((n_row, heads_here * rows, width), f32),
            pltpu.VMEM((owners, per_owner, heads_here * rows, width), f32),
            pltpu.VMEM(att_w.shape, bf16),
            pltpu.VMEM((n_sub, spread, width), bf16),
            pltpu.VMEM((rows, half, width), bf16),
            pltpu.VMEM((rows, half, width), f32),
            pltpu.VMEM((n_row, rows, half, width), bf16),
            pltpu.VMEM((rows, half, width), f32),
            pltpu.VMEM((2, rows * rows, width), f32),
            pltpu.VMEM((n_row, rows * rows, width), bf16),
            pltpu.VMEM((owners, per_owner, rows * rows, width), bf16),
            pltpu.VMEM((rows, half, width), f32),
            pltpu.VMEM((rows * half, width), f32),
            dma((2, 2, 2)),
            dma((2, 2, 2)),
            dma((2,)),
            dma((2,)),
            dma((n_row // STRIDE, len(LOCAL) + 2)),
            dma((n_row,)),
            dma((n_row,)),
            dma((owners, per_owner)),
            dma((2, 2, CHUNKS)),
            dma((2, n_row // 2, CHUNKS)),
            dma((n_row,)),
            dma((owners, per_owner)),
        ],
        compiler_params=pltpu.CompilerParams(collective_id=0, has_side_effects=True),
    )(
        length,
        chain,
        chain_bias,
        pair,
        chain_cols,
        bias_w,
        att_w,
        att_out,
        mult_in,
        mult_gate,
        mult_out,
        trans_up,
        trans_down,
    )


def solution(mesh):
    placed = (
        P(("grp", "row"), "col", None),
        P("grp"),
        P("grp"),
        P(None, None, "sub"),
        P(None, "sub"),
        P("sub"),
        P("sub", None),
        P(),
        P(),
        P(),
        P(),
        P(),
    )
    return jax.shard_map(
        local,
        mesh=mesh,
        in_specs=placed,
        out_specs=P(("grp", "row"), ("col", "sub"), None),
        check_vma=False,
    )
```

```python
import functools

import jax
import jax.numpy as jnp
from jax import lax
from jax.experimental import pallas as pl
from jax.experimental.pallas import tpu as pltpu
from jax.sharding import PartitionSpec as P

MESH = pl.DeviceIdType.MESH
CHUNKS = 4
STRIDE = 4
LOCAL = (-1, 1, 2)


def norm(value):
    mean = jnp.mean(value, axis=-1, keepdims=True)
    centred = value - mean
    variance = jnp.mean(centred * centred, axis=-1, keepdims=True)
    return centred * lax.rsqrt(variance + 1e-05)


def pair_kernel(
    n_row,
    n_col,
    n_sub,
    length_ref,
    chain_ref,
    chain_bias_ref,
    pair_ref,
    chain_lanes_ref,
    att_bias_ref,
    att_w_ref,
    att_out_ref,
    mult_in_ref,
    mult_gate_ref,
    mult_out_ref,
    trans_up_ref,
    trans_down_ref,
    out_ref,
    normed,
    kept,
    queries,
    att_gate,
    scores,
    bias,
    pieces,
    bias_in,
    both_w,
    both_out,
    attended,
    first_ref,
    gathered,
    left,
    stage_f32,
    stage,
    parts,
    tri,
    gate,
    x_send,
    x_recv,
    weight_send,
    weight_recv,
    chain_send,
    chain_recv,
    bias_send,
    bias_recv,
    ring_send,
    ring_recv,
    part_send,
    part_recv,
):
    rows, cols, width = pair_ref.shape
    half = cols // n_sub
    total = rows * n_row
    piece = rows // CHUNKS
    block_rows = rows // 2
    heads_here = pieces.shape[1] // rows
    heads = heads_here * n_sub
    head_dim = width // heads
    z = lax.axis_index("row")
    x = lax.axis_index("col")
    core = lax.axis_index("sub")
    owners = n_col * n_sub
    me = x * n_sub + core
    per_owner = n_row // owners
    far = n_row // 2
    up = lax.rem(z + 1, n_row)
    down = lax.rem(z + n_row - 1, n_row)
    length = length_ref[0]

    def row_at(offset):
        return lax.rem(z + (offset + n_row), n_row)

    barrier = pltpu.get_barrier_semaphore()
    near = (1, -1, 2, -2, STRIDE, -STRIDE)
    for offset in near:
        pl.semaphore_signal(
            barrier, inc=1, device_id={"row": row_at(offset)}, device_id_type=MESH
        )
    for step in range(1, owners):
        other = lax.rem(me + step, owners)
        pl.semaphore_signal(
            barrier,
            inc=1,
            device_id={"col": lax.div(other, n_sub), "sub": lax.rem(other, n_sub)},
            device_id_type=MESH,
        )

    normed[x] = norm(pair_ref[...].astype(jnp.float32)).astype(jnp.bfloat16)
    both_out[core] = att_out_ref[...]
    both_w[core] = att_w_ref[...]

    lane = lax.broadcasted_iota(jnp.int32, (1, width), 1)
    begin = x * cols
    turn = lax.rem(begin, width)
    key = begin + lax.rem(lane + (width - turn), width)
    key_chain = jnp.zeros((1, width), jnp.int32)
    for k in range(total // width):
        held = chain_lanes_ref[:, k * width : (k + 1) * width]
        key_chain = jnp.where(key // width == k, held, key_chain)
    key_bias = ((key < length).astype(jnp.float32) - 1.0) * 1000000000.0
    padding = jnp.zeros((width - cols, width), jnp.bfloat16)
    bias_w = att_bias_ref[...]
    for i in range(rows):
        keys_i = jnp.concatenate([normed[x, i], padding], axis=0)
        term = lax.dot_general(
            bias_w, keys_i, (((1,), (1,)), ((), ())), preferred_element_type=jnp.float32
        )
        term = pltpu.roll(term, turn, 1)
        same = (key_chain == chain_ref[z * rows + i]).astype(jnp.float32)
        for h in range(heads_here):
            at = h * rows + i
            pieces[z, at : at + 1] = term[h : h + 1] + chain_bias_ref[h] * same + key_bias

    pl.semaphore_wait(barrier, len(near) + owners - 1)

    def weight_copy(k):
        source, target = [
            (att_w_ref, both_w.at[core]),
            (att_out_ref, both_out.at[core]),
        ][k]
        return pltpu.make_async_remote_copy(
            src_ref=source,
            dst_ref=target,
            send_sem=weight_send.at[k],
            recv_sem=weight_recv.at[k],
            device_id={"sub": 1 - core},
            device_id_type=MESH,
        )

    def x_copy(way, step, chunk, arrives):
        distance = step + 1 if arrives else step
        source = lax.rem(x + (n_col - distance if way == 0 else distance), n_col)
        block = normed.at[source, pl.ds(chunk * block_rows, block_rows)]
        return pltpu.make_async_remote_copy(
            src_ref=block,
            dst_ref=block,
            send_sem=x_send.at[way, step, chunk],
            recv_sem=x_recv.at[way, step, chunk],
            device_id={"col": lax.rem(x + (1 if way == 0 else n_col - 1), n_col)},
            device_id_type=MESH,
        )

    def bias_hop(stop, k, block, offset):
        return pltpu.make_async_remote_copy(
            src_ref=pieces.at[block],
            dst_ref=pieces.at[block],
            send_sem=chain_send.at[stop, k],
            recv_sem=chain_recv.at[block],
            device_id={"row": row_at(offset)},
            device_id_type=MESH,
        )

    def owner_copy(block, source, target, send_sem, recv_sem):
        dest = lax.div(block, per_owner)
        return pltpu.make_async_remote_copy(
            src_ref=source.at[block],
            dst_ref=target.at[me, lax.rem(block, per_owner)],
            send_sem=send_sem.at[block],
            recv_sem=recv_sem.at[me, lax.rem(block, per_owner)],
            device_id={"col": lax.div(dest, n_sub), "sub": lax.rem(dest, n_sub)},
            device_id_type=MESH,
        )

    def to_owner(block, source, target, send_sem, recv_sem):
        slot = lax.rem(block, per_owner)
        mine = lax.div(block, per_owner) == me

        @pl.when(mine)
        def _():
            pltpu.make_async_copy(
                source.at[block], target.at[me, slot], recv_sem.at[me, slot]
            ).start()

        @pl.when(jnp.logical_not(mine))
        def _():
            owner_copy(block, source, target, send_sem, recv_sem).start()

    bias_way = (pieces, bias_in, bias_send, bias_recv)
    part_way = (stage, parts, part_send, part_recv)
    ups = n_row // (2 * STRIDE)

    def hops_of(stop):
        if stop == 0:
            ahead = [(0, STRIDE), (len(LOCAL) + 1, -STRIDE)]
        elif stop < ups:
            ahead = [(0, STRIDE)]
        elif stop == ups or stop == 2 * ups - 1:
            ahead = []
        else:
            ahead = [(0, -STRIDE)]
        return ahead + [(1 + n, offset) for n, offset in enumerate(LOCAL)]

    def block_of(stop):
        return row_at(-STRIDE * stop if stop <= ups else STRIDE * (stop - ups))

    def pass_on(stop):
        block = block_of(stop)
        if stop > 0:
            bias_hop(stop, 0, block, 0).wait_recv()
        for k, offset in hops_of(stop):
            bias_hop(stop, k, block, offset).start()
        to_owner(block, *bias_way)

    def take_local(stop):
        for offset in LOCAL:
            block = lax.rem(block_of(stop) + (n_row - offset), n_row)
            bias_hop(stop, 0, block, 0).wait_recv()
            to_owner(block, *bias_way)

    def project(source, chunk):
        tile = normed[source, pl.ds(chunk * block_rows, block_rows)]
        made = times(tile.reshape(block_rows * cols, width), w_kept).astype(jnp.bfloat16)
        kept[
            pl.ds(chunk * block_rows, block_rows), pl.ds(pl.multiple_of(source * cols, 32), cols)
        ] = made.reshape(block_rows, cols, 2 * width)

    def score(i, carry):
        scores[i] = lax.dot_general(
            queries[i],
            kept[i, :, :width],
            (((1,), (1,)), ((), ())),
            preferred_element_type=jnp.float32,
        )
        return carry

    pass_on(0)
    for k in range(2):
        weight_copy(k).start()
    for chunk in range(2):
        for way in range(2):
            x_copy(way, 0, chunk if way == 0 else 1 - chunk, False).start()

    for k in range(2):
        weight_copy(k).wait_recv()

    def joined(g):
        return jnp.concatenate([both_w[k, g] for k in range(n_sub)], axis=0)

    def times(value, weight):
        return lax.dot_general(
            value, weight, (((1,), (1,)), ((), ())), preferred_element_type=jnp.float32
        )

    w_query, w_gate = joined(0), joined(3)
    w_kept = jnp.concatenate([joined(1), joined(2)], axis=0)
    tile = normed[x, :, pl.ds(pl.multiple_of(core * half, 16), half)].reshape(rows * half, width)
    query = (times(tile, w_query) * head_dim ** (-0.5)).astype(jnp.bfloat16)
    head_of = lax.broadcasted_iota(jnp.int32, (rows * half, width), 1) // head_dim
    for h in range(heads):
        queries[:, h * half : (h + 1) * half] = jnp.where(
            head_of == h, query, jnp.zeros_like(query)
        ).reshape(rows, half, width)
    att_gate[...] = jax.nn.sigmoid(times(tile, w_gate)).reshape(rows, half, width)
    for chunk in range(2):
        project(x, chunk)

    x_up = lax.rem(x + n_col - 1, n_col)
    x_down = lax.rem(x + 1, n_col)
    x_far = lax.rem(x + 2, n_col)

    def stage_of(step):
        if step <= ups:
            pass_on(step)
        if step < ups:
            pass_on(ups + step)
        take_local(step - 1)
        if 1 <= step - 1 < ups:
            take_local(ups + step - 1)

    stage_of(1)
    x_copy(0, 0, 0, True).wait_recv()
    x_copy(0, 1, 0, False).start()
    x_copy(1, 0, 1, True).wait_recv()
    x_copy(1, 1, 1, False).start()
    project(x_up, 0)
    project(x_down, 1)
    stage_of(2)
    x_copy(0, 0, 1, True).wait_recv()
    project(x_up, 1)
    x_copy(1, 0, 0, True).wait_recv()
    project(x_down, 0)
    stage_of(3)
    x_copy(0, 1, 0, True).wait_recv()
    project(x_far, 0)
    lax.fori_loop(0, block_rows, score, 0)
    stage_of(4)
    x_copy(1, 1, 1, True).wait_recv()
    project(x_far, 1)
    lax.fori_loop(block_rows, rows, score, 0)
    take_local(ups)

    for slot in range(per_owner):
        for giver in range(owners):
            pltpu.make_async_copy(
                pieces.at[0], bias_in.at[giver, slot], bias_recv.at[giver, slot]
            ).wait()
    lane = lax.broadcasted_iota(jnp.int32, (rows, width), 1)
    for slot in range(per_owner):
        for h in range(heads):
            giver, own_head = h // heads_here, h % heads_here
            held = [
                bias_in[k * n_sub + giver, slot, own_head * rows : (own_head + 1) * rows]
                for k in range(n_col)
            ]
            at = h * half + slot * rows
            for k in range(total // width):
                line = None
                for source in range(n_col):
                    begin = source * cols - k * width
                    if begin + cols <= 0 or begin >= width:
                        continue
                    line = held[source] if line is None else jnp.where(lane >= begin, held[source], line)
                bias[at : at + rows, k * width : (k + 1) * width] = line

    head_of = lax.broadcasted_iota(jnp.int32, (half, width), 1) // head_dim

    def attend(i, carry):
        logits = scores[i] + bias[...]
        weights = jnp.exp(logits - jnp.max(logits, axis=-1, keepdims=True))
        weights = weights * (1.0 / jnp.sum(weights, axis=-1, keepdims=True))
        mixed_values = jnp.dot(
            weights.astype(jnp.bfloat16), kept[i, :, width:], preferred_element_type=jnp.float32
        )
        taken = jnp.zeros((half, width), jnp.float32)
        for h in range(heads):
            taken = jnp.where(head_of == h, mixed_values[h * half : (h + 1) * half], taken)
        attended[i] = (taken * att_gate[i]).astype(jnp.bfloat16)
        return carry

    lax.fori_loop(0, rows, attend, 0, unroll=2)
    first_ref[...] = pair_ref[:, pl.ds(pl.multiple_of(core * half, 16), half)].astype(
        jnp.float32
    ) + jnp.dot(
        attended[...].reshape(rows * half, width),
        both_out[...].reshape(width, width),
        preferred_element_type=jnp.float32,
    ).reshape(rows, half, width)

    first = first_ref[...].reshape(rows * half, width)
    mixed = norm(first).astype(jnp.bfloat16)
    quad = jnp.dot(mixed, mult_in_ref[...], preferred_element_type=jnp.float32)
    shape = (rows, half, width)
    here_row = z * rows + lax.broadcasted_iota(jnp.int32, shape, 0)
    here_col = (x * n_sub + core) * half + lax.broadcasted_iota(jnp.int32, shape, 1)
    valid = ((here_row < length) & (here_col < length)).astype(jnp.float32)
    a, b, c, d = [quad[:, k * width : (k + 1) * width].reshape(shape) for k in range(4)]
    left[...] = (valid * jax.nn.sigmoid(b) * a).astype(jnp.bfloat16).astype(jnp.float32)
    gathered[z] = (valid * jax.nn.sigmoid(d) * c).astype(jnp.bfloat16)
    gate[...] = jax.nn.sigmoid(
        jnp.dot(mixed, mult_gate_ref[...], preferred_element_type=jnp.float32)
    )

    def source(way, step):
        return lax.rem(z + (n_row - step if way == 0 else step), n_row)

    def ring_copy(way, step, chunk, arrives):
        block = gathered.at[source(way, step), pl.ds(chunk * piece, piece)]
        return pltpu.make_async_remote_copy(
            src_ref=block,
            dst_ref=block,
            send_sem=ring_send.at[way, lax.rem(step, 2), chunk],
            recv_sem=ring_recv.at[way, step - 1 if arrives else step, chunk],
            device_id={"row": up if way == 0 else down},
            device_id_type=MESH,
        )

    def hop(way, step, chunk):
        return ring_copy(way, step, chunk, False)

    def arrival(way, step, chunk):
        return ring_copy(way, step, chunk, True)

    def multiply(owner, chunk, lane):
        for jj in range(piece):
            j = chunk * piece + jj
            right = gathered[owner, j].astype(jnp.float32)
            for i in range(rows):
                stage_f32[lane, pl.ds(i * rows + j, 1)] = jnp.sum(
                    left[i] * right, axis=0, keepdims=True
                )

    def give(block, lane):
        stage[block] = stage_f32[lane].astype(jnp.bfloat16)
        to_owner(block, *part_way)

    for chunk in range(CHUNKS):
        for way in range(2):
            hop(way, 0, chunk).start()

    def own(chunk, carry):
        multiply(z, chunk, 0)
        return carry

    lax.fori_loop(0, CHUNKS, own, 0)
    give(z, 0)

    def visit(n, carry):
        step = lax.div(n, CHUNKS) + 1
        chunk = lax.rem(n, CHUNKS)
        for way in range(2):
            arrival(way, step, chunk).wait_recv()
            last = chunk < CHUNKS // 2 if way == 0 else chunk >= CHUNKS // 2

            @pl.when(step >= 2)
            def _():
                hop(way, step, chunk).wait_send()

            @pl.when(jnp.logical_or(step < far - 1, last))
            def _():
                hop(way, step, chunk).start()

        for way in range(2):
            multiply(source(way, step), chunk, way)

        @pl.when(chunk == CHUNKS - 1)
        def _():
            for way in range(2):
                give(source(way, step), way)

        return carry

    lax.fori_loop(0, (far - 1) * CHUNKS, visit, 0)

    for chunk in range(CHUNKS):
        arrival(0 if chunk < CHUNKS // 2 else 1, far, chunk).wait_recv()
        multiply(source(0, far), chunk, 0)
    give(source(0, far), 0)

    for way in range(2):
        for chunk in range(CHUNKS):
            hop(way, far - 2, chunk).wait_send()
            if (chunk < CHUNKS // 2) == (way == 0):
                hop(way, far - 1, chunk).wait_send()

    for stop in range(2 * ups):
        for k, offset in hops_of(stop):
            bias_hop(stop, k, block_of(stop), offset).wait_send()
    for k in range(2):
        weight_copy(k).wait_send()
    for way in range(2):
        for chunk in range(2):
            x_copy(way, 0, chunk, False).wait_send()
        x_copy(way, 1, way, False).wait_send()

    def sent(block, carry):
        @pl.when(lax.div(block, per_owner) != me)
        def _():
            owner_copy(block, *bias_way).wait_send()
            owner_copy(block, *part_way).wait_send()

        return carry

    lax.fori_loop(0, n_row, sent, 0)

    for slot in range(per_owner):
        total_f32 = None
        for giver in range(owners):
            pltpu.make_async_copy(
                stage.at[0], parts.at[giver, slot], part_recv.at[giver, slot]
            ).wait()
            part = parts[giver, slot].astype(jnp.float32)
            total_f32 = part if total_f32 is None else total_f32 + part
        for i in range(rows):
            tri[i, slot * rows : (slot + 1) * rows] = total_f32[i * rows : (i + 1) * rows]

    tri_normed = norm(tri[...].reshape(rows * half, width)).astype(jnp.bfloat16)
    second = first_ref[...].reshape(rows * half, width) + gate[...] * jnp.dot(
        tri_normed, mult_out_ref[...], preferred_element_type=jnp.float32
    )
    last_normed = norm(second).astype(jnp.bfloat16)
    hidden = jax.nn.relu(
        jnp.dot(last_normed, trans_up_ref[...], preferred_element_type=jnp.float32)
    ).astype(jnp.bfloat16)
    result = second + jnp.dot(hidden, trans_down_ref[...], preferred_element_type=jnp.float32)
    out_ref[...] = result.astype(jnp.bfloat16).reshape(rows, half, width)


def local(
    pair,
    length,
    chain,
    att_proj,
    att_bias,
    chain_bias,
    att_out,
    mult_in,
    mult_gate,
    mult_out,
    trans_up,
    trans_down,
):
    rows, cols, width = pair.shape
    n_row, n_col, n_sub = (lax.axis_size(a) for a in ("row", "col", "sub"))
    owners = n_col * n_sub
    per_owner = n_row // owners
    half = cols // n_sub
    total = rows * n_row
    heads_here = att_bias.shape[1]
    heads = heads_here * n_sub
    spread = att_out.shape[0]
    vmem = pl.BlockSpec(memory_space=pltpu.VMEM)
    smem = pl.BlockSpec(memory_space=pltpu.SMEM)
    dma = pltpu.SemaphoreType.DMA
    bf16, f32 = jnp.bfloat16, jnp.float32
    return pl.pallas_call(
        functools.partial(pair_kernel, n_row, n_col, n_sub),
        out_shape=jax.ShapeDtypeStruct((rows, half, width), bf16),
        in_specs=[smem] * 3 + [vmem] * 10,
        out_specs=vmem,
        scratch_shapes=[
            pltpu.VMEM((n_col, rows, cols, width), bf16),
            pltpu.VMEM((rows, total, 2 * width), bf16),
            pltpu.VMEM((rows, heads * half, width), bf16),
            pltpu.VMEM((rows, half, width), f32),
            pltpu.VMEM((rows, heads * half, total), f32),
            pltpu.VMEM((heads * half, total), f32),
            pltpu.VMEM((n_row, heads_here * rows, width), f32),
            pltpu.VMEM((owners, per_owner, heads_here * rows, width), f32),
            pltpu.VMEM((n_sub, 4, spread, width), bf16),
            pltpu.VMEM((n_sub, spread, width), bf16),
            pltpu.VMEM((rows, half, width), bf16),
            pltpu.VMEM((rows, half, width), f32),
            pltpu.VMEM((n_row, rows, half, width), bf16),
            pltpu.VMEM((rows, half, width), f32),
            pltpu.VMEM((2, rows * rows, width), f32),
            pltpu.VMEM((n_row, rows * rows, width), bf16),
            pltpu.VMEM((owners, per_owner, rows * rows, width), bf16),
            pltpu.VMEM((rows, half, width), f32),
            pltpu.VMEM((rows * half, width), f32),
            dma((2, 2, 2)),
            dma((2, 2, 2)),
            dma((2,)),
            dma((2,)),
            dma((n_row // STRIDE, len(LOCAL) + 2)),
            dma((n_row,)),
            dma((n_row,)),
            dma((owners, per_owner)),
            dma((2, 2, CHUNKS)),
            dma((2, n_row // 2, CHUNKS)),
            dma((n_row,)),
            dma((owners, per_owner)),
        ],
        compiler_params=pltpu.CompilerParams(collective_id=0, has_side_effects=True),
    )(
        length,
        chain,
        chain_bias,
        pair,
        chain[None],
        att_bias.T,
        att_proj.transpose(1, 2, 0),
        att_out,
        mult_in,
        mult_gate,
        mult_out,
        trans_up,
        trans_down,
    )


def solution(mesh):
    placed = (
        P(("grp", "row"), "col", None),
        P("grp"),
        P("grp"),
        P(None, None, "sub"),
        P(None, "sub"),
        P("sub"),
        P("sub", None),
        P(),
        P(),
        P(),
        P(),
        P(),
    )
    return jax.shard_map(
        local,
        mesh=mesh,
        in_specs=placed,
        out_specs=P(("grp", "row"), ("col", "sub"), None),
        check_vma=False,
    )
```

```python
import functools

import jax
import jax.numpy as jnp
from jax import lax
from jax.experimental import pallas as pl
from jax.experimental.pallas import tpu as pltpu
from jax.sharding import PartitionSpec as P

MESH = pl.DeviceIdType.MESH
CHUNKS = 4
STRIDE = 4


def norm(value):
    mean = jnp.mean(value, axis=-1, keepdims=True)
    centred = value - mean
    variance = jnp.mean(centred * centred, axis=-1, keepdims=True)
    return centred * lax.rsqrt(variance + 1e-05)


def pair_kernel(
    n_row,
    n_col,
    n_sub,
    length_ref,
    chain_ref,
    chain_bias_ref,
    pair_ref,
    chain_lanes_ref,
    att_bias_ref,
    att_w_ref,
    att_out_ref,
    mult_in_ref,
    mult_gate_ref,
    mult_out_ref,
    trans_up_ref,
    trans_down_ref,
    out_ref,
    normed,
    kept,
    queries,
    att_gate,
    scores,
    bias,
    pieces,
    bias_in,
    both_w,
    both_out,
    attended,
    first_ref,
    gathered,
    left,
    stage_f32,
    stage,
    parts,
    tri,
    gate,
    x_send,
    x_recv,
    weight_send,
    weight_recv,
    chain_send,
    direct_send,
    chain_recv,
    bias_send,
    bias_recv,
    ring_send,
    ring_recv,
    part_send,
    part_recv,
):
    rows, cols, width = pair_ref.shape
    half = cols // n_sub
    total = rows * n_row
    piece = rows // CHUNKS
    block_rows = rows // 2
    heads_here = pieces.shape[1] // rows
    heads = heads_here * n_sub
    head_dim = width // heads
    z = lax.axis_index("row")
    x = lax.axis_index("col")
    core = lax.axis_index("sub")
    owners = n_col * n_sub
    me = x * n_sub + core
    per_owner = n_row // owners
    far = n_row // 2
    up = lax.rem(z + 1, n_row)
    down = lax.rem(z + n_row - 1, n_row)
    length = length_ref[0]

    def greet(other):
        pl.semaphore_signal(barrier, inc=1, device_id={"row": other}, device_id_type=MESH)

    barrier = pltpu.get_barrier_semaphore()
    for offset in range(1, STRIDE + 1):

        @pl.when(z >= offset)
        def _():
            greet(z - offset)

    def greet_later(other, carry):
        greet(other)
        return carry

    lax.fori_loop(z + 1, n_row, greet_later, 0)

    @pl.when(z == n_row - 1)
    def _():
        greet(0)

    for step in range(1, owners):
        other = lax.rem(me + step, owners)
        pl.semaphore_signal(
            barrier,
            inc=1,
            device_id={"col": lax.div(other, n_sub), "sub": lax.rem(other, n_sub)},
            device_id_type=MESH,
        )

    normed[x] = norm(pair_ref[...].astype(jnp.float32)).astype(jnp.bfloat16)
    both_out[core] = att_out_ref[...]
    both_w[core] = att_w_ref[...]

    lane = lax.broadcasted_iota(jnp.int32, (1, width), 1)
    begin = x * cols
    turn = lax.rem(begin, width)
    key = begin + lax.rem(lane + (width - turn), width)
    key_chain = jnp.zeros((1, width), jnp.int32)
    for k in range(total // width):
        held = chain_lanes_ref[k * width : (k + 1) * width].reshape(1, width)
        key_chain = jnp.where(key // width == k, held, key_chain)
    key_bias = ((key < length).astype(jnp.float32) - 1.0) * 1000000000.0
    padding = jnp.zeros((width - cols, width), jnp.bfloat16)
    bias_w = att_bias_ref[...]
    for i in range(rows):
        keys_i = jnp.concatenate([normed[x, i], padding], axis=0)
        term = lax.dot_general(
            bias_w, keys_i, (((1,), (1,)), ((), ())), preferred_element_type=jnp.float32
        )
        term = pltpu.roll(term, turn, 1)
        same = (key_chain == chain_ref[z * rows + i]).astype(jnp.float32)
        for h in range(heads_here):
            at = h * rows + i
            pieces[z, at : at + 1] = term[h : h + 1] + chain_bias_ref[h] * same + key_bias

    ends = jnp.where(z == 0, 1, 0)
    after = jnp.minimum(n_row - 1 - z, STRIDE)
    pl.semaphore_wait(barrier, z + after + ends + owners - 1)

    def weight_copy(k):
        source, target = [
            (att_w_ref, both_w.at[core]),
            (att_out_ref, both_out.at[core]),
        ][k]
        return pltpu.make_async_remote_copy(
            src_ref=source,
            dst_ref=target,
            send_sem=weight_send.at[k],
            recv_sem=weight_recv.at[k],
            device_id={"sub": 1 - core},
            device_id_type=MESH,
        )

    def x_copy(way, step, chunk, arrives):
        distance = step + 1 if arrives else step
        source = lax.rem(x + (n_col - distance if way == 0 else distance), n_col)
        block = normed.at[source, pl.ds(chunk * block_rows, block_rows)]
        return pltpu.make_async_remote_copy(
            src_ref=block,
            dst_ref=block,
            send_sem=x_send.at[way, step, chunk],
            recv_sem=x_recv.at[way, step, chunk],
            device_id={"col": lax.rem(x + (1 if way == 0 else n_col - 1), n_col)},
            device_id_type=MESH,
        )

    def bias_hop(block, target, send_sem):
        return pltpu.make_async_remote_copy(
            src_ref=pieces.at[block],
            dst_ref=pieces.at[block],
            send_sem=send_sem,
            recv_sem=chain_recv.at[block],
            device_id={"row": target},
            device_id_type=MESH,
        )

    def direct(target):
        return bias_hop(z, target, direct_send.at[target])

    def relay(block, offset):
        return bias_hop(
            block, z + offset, chain_send.at[lax.div(block, STRIDE), offset - 1]
        )

    def each_relay(block, act):
        for offset in range(STRIDE, 0, -1):

            @pl.when(z + offset < n_row)
            def _():
                act(relay(block, offset))

    def owner_copy(block, source, target, send_sem, recv_sem):
        dest = lax.div(block, per_owner)
        return pltpu.make_async_remote_copy(
            src_ref=source.at[block],
            dst_ref=target.at[me, lax.rem(block, per_owner)],
            send_sem=send_sem.at[block],
            recv_sem=recv_sem.at[me, lax.rem(block, per_owner)],
            device_id={"col": lax.div(dest, n_sub), "sub": lax.rem(dest, n_sub)},
            device_id_type=MESH,
        )

    def to_owner(block, source, target, send_sem, recv_sem):
        slot = lax.rem(block, per_owner)
        mine = lax.div(block, per_owner) == me

        @pl.when(mine)
        def _():
            pltpu.make_async_copy(
                source.at[block], target.at[me, slot], recv_sem.at[me, slot]
            ).start()

        @pl.when(jnp.logical_not(mine))
        def _():
            owner_copy(block, source, target, send_sem, recv_sem).start()

    bias_way = (pieces, bias_in, bias_send, bias_recv)
    part_way = (stage, parts, part_send, part_recv)

    def own_bias():
        each_relay(z, lambda copy: copy.start())

        def send(n, carry):
            distance = far - n

            @pl.when(z >= distance)
            def _():
                direct(z - distance).start()

            @pl.when(jnp.logical_and(z + distance >= n_row, distance < far))
            def _():
                direct(z + distance - n_row).start()

            return carry

        lax.fori_loop(0, far, send, 0)
        to_owner(z, *bias_way)

    def take_earlier(block, carry):
        bias_hop(block, z, chain_send.at[0, 0]).wait_recv()

        @pl.when(lax.rem(z - block, STRIDE) == 0)
        def _():
            each_relay(block, lambda copy: copy.start())

        to_owner(block, *bias_way)
        return carry

    def take_later(block, carry):
        bias_hop(block, z, chain_send.at[0, 0]).wait_recv()
        to_owner(block, *bias_way)
        return carry

    def project(source, chunk):
        tile = normed[source, pl.ds(chunk * block_rows, block_rows)]
        made = times(tile.reshape(block_rows * cols, width), w_kept).astype(jnp.bfloat16)
        kept[
            pl.ds(chunk * block_rows, block_rows), pl.ds(pl.multiple_of(source * cols, 32), cols)
        ] = made.reshape(block_rows, cols, 2 * width)

    def score(i, carry):
        scores[i] = lax.dot_general(
            queries[i],
            kept[i, :, :width],
            (((1,), (1,)), ((), ())),
            preferred_element_type=jnp.float32,
        )
        return carry

    own_bias()
    for k in range(2):
        weight_copy(k).start()
    for chunk in range(2):
        for way in range(2):
            x_copy(way, 0, chunk if way == 0 else 1 - chunk, False).start()

    for k in range(2):
        weight_copy(k).wait_recv()

    def joined(g):
        return jnp.concatenate([both_w[k, g] for k in range(n_sub)], axis=0)

    def times(value, weight):
        return lax.dot_general(
            value, weight, (((1,), (1,)), ((), ())), preferred_element_type=jnp.float32
        )

    w_query, w_gate = joined(0), joined(3)
    w_kept = jnp.concatenate([joined(1), joined(2)], axis=0)
    tile = normed[x, :, pl.ds(pl.multiple_of(core * half, 16), half)].reshape(rows * half, width)
    query = (times(tile, w_query) * head_dim ** (-0.5)).astype(jnp.bfloat16)
    head_of = lax.broadcasted_iota(jnp.int32, (rows * half, width), 1) // head_dim
    for h in range(heads):
        queries[:, h * half : (h + 1) * half] = jnp.where(
            head_of == h, query, jnp.zeros_like(query)
        ).reshape(rows, half, width)
    att_gate[...] = jax.nn.sigmoid(times(tile, w_gate)).reshape(rows, half, width)
    for chunk in range(2):
        project(x, chunk)

    x_up = lax.rem(x + n_col - 1, n_col)
    x_down = lax.rem(x + 1, n_col)
    x_far = lax.rem(x + 2, n_col)

    x_copy(0, 0, 0, True).wait_recv()
    x_copy(0, 1, 0, False).start()
    x_copy(1, 0, 1, True).wait_recv()
    x_copy(1, 1, 1, False).start()
    project(x_up, 0)
    project(x_down, 1)
    lax.fori_loop(0, z, take_earlier, 0)
    x_copy(0, 0, 1, True).wait_recv()
    project(x_up, 1)
    x_copy(1, 0, 0, True).wait_recv()
    project(x_down, 0)
    x_copy(0, 1, 0, True).wait_recv()
    project(x_far, 0)
    lax.fori_loop(0, block_rows, score, 0)
    x_copy(1, 1, 1, True).wait_recv()
    project(x_far, 1)
    lax.fori_loop(block_rows, rows, score, 0)
    lax.fori_loop(z + 1, n_row, take_later, 0)

    for slot in range(per_owner):
        for giver in range(owners):
            pltpu.make_async_copy(
                pieces.at[0], bias_in.at[giver, slot], bias_recv.at[giver, slot]
            ).wait()
    lane = lax.broadcasted_iota(jnp.int32, (rows, width), 1)
    for slot in range(per_owner):
        for h in range(heads):
            giver, own_head = h // heads_here, h % heads_here
            held = [
                bias_in[k * n_sub + giver, slot, own_head * rows : (own_head + 1) * rows]
                for k in range(n_col)
            ]
            at = h * half + slot * rows
            for k in range(total // width):
                line = None
                for source in range(n_col):
                    begin = source * cols - k * width
                    if begin + cols <= 0 or begin >= width:
                        continue
                    line = held[source] if line is None else jnp.where(lane >= begin, held[source], line)
                bias[at : at + rows, k * width : (k + 1) * width] = line

    head_of = lax.broadcasted_iota(jnp.int32, (half, width), 1) // head_dim

    def attend(i, carry):
        logits = scores[i] + bias[...]
        weights = jnp.exp(logits - jnp.max(logits, axis=-1, keepdims=True))
        weights = weights * (1.0 / jnp.sum(weights, axis=-1, keepdims=True))
        mixed_values = jnp.dot(
            weights.astype(jnp.bfloat16), kept[i, :, width:], preferred_element_type=jnp.float32
        )
        taken = jnp.zeros((half, width), jnp.float32)
        for h in range(heads):
            taken = jnp.where(head_of == h, mixed_values[h * half : (h + 1) * half], taken)
        attended[i] = (taken * att_gate[i]).astype(jnp.bfloat16)
        return carry

    lax.fori_loop(0, rows, attend, 0, unroll=2)
    first_ref[...] = pair_ref[:, pl.ds(pl.multiple_of(core * half, 16), half)].astype(
        jnp.float32
    ) + jnp.dot(
        attended[...].reshape(rows * half, width),
        both_out[...].reshape(width, width),
        preferred_element_type=jnp.float32,
    ).reshape(rows, half, width)

    first = first_ref[...].reshape(rows * half, width)
    mixed = norm(first).astype(jnp.bfloat16)
    quad = jnp.dot(mixed, mult_in_ref[...], preferred_element_type=jnp.float32)
    shape = (rows, half, width)
    here_row = z * rows + lax.broadcasted_iota(jnp.int32, shape, 0)
    here_col = (x * n_sub + core) * half + lax.broadcasted_iota(jnp.int32, shape, 1)
    valid = ((here_row < length) & (here_col < length)).astype(jnp.float32)
    a, b, c, d = [quad[:, k * width : (k + 1) * width].reshape(shape) for k in range(4)]
    left[...] = (valid * jax.nn.sigmoid(b) * a).astype(jnp.bfloat16).astype(jnp.float32)
    gathered[z] = (valid * jax.nn.sigmoid(d) * c).astype(jnp.bfloat16)
    gate[...] = jax.nn.sigmoid(
        jnp.dot(mixed, mult_gate_ref[...], preferred_element_type=jnp.float32)
    )

    def source(way, step):
        return lax.rem(z + (n_row - step if way == 0 else step), n_row)

    def ring_copy(way, step, chunk, arrives):
        block = gathered.at[source(way, step), pl.ds(chunk * piece, piece)]
        return pltpu.make_async_remote_copy(
            src_ref=block,
            dst_ref=block,
            send_sem=ring_send.at[way, lax.rem(step, 2), chunk],
            recv_sem=ring_recv.at[way, step - 1 if arrives else step, chunk],
            device_id={"row": up if way == 0 else down},
            device_id_type=MESH,
        )

    def hop(way, step, chunk):
        return ring_copy(way, step, chunk, False)

    def arrival(way, step, chunk):
        return ring_copy(way, step, chunk, True)

    def multiply(owner, chunk, lane):
        for jj in range(piece):
            j = chunk * piece + jj
            right = gathered[owner, j].astype(jnp.float32)
            for i in range(rows):
                stage_f32[lane, pl.ds(i * rows + j, 1)] = jnp.sum(
                    left[i] * right, axis=0, keepdims=True
                )

    def give(block, lane):
        stage[block] = stage_f32[lane].astype(jnp.bfloat16)
        to_owner(block, *part_way)

    for chunk in range(CHUNKS):
        for way in range(2):
            hop(way, 0, chunk).start()

    def own(chunk, carry):
        multiply(z, chunk, 0)
        return carry

    lax.fori_loop(0, CHUNKS, own, 0)
    give(z, 0)

    def visit(n, carry):
        step = lax.div(n, CHUNKS) + 1
        chunk = lax.rem(n, CHUNKS)
        for way in range(2):
            arrival(way, step, chunk).wait_recv()
            last = chunk < CHUNKS // 2 if way == 0 else chunk >= CHUNKS // 2

            @pl.when(step >= 2)
            def _():
                hop(way, step, chunk).wait_send()

            @pl.when(jnp.logical_or(step < far - 1, last))
            def _():
                hop(way, step, chunk).start()

        for way in range(2):
            multiply(source(way, step), chunk, way)

        @pl.when(chunk == CHUNKS - 1)
        def _():
            for way in range(2):
                give(source(way, step), way)

        return carry

    lax.fori_loop(0, (far - 1) * CHUNKS, visit, 0)

    for chunk in range(CHUNKS):
        arrival(0 if chunk < CHUNKS // 2 else 1, far, chunk).wait_recv()
        multiply(source(0, far), chunk, 0)
    give(source(0, far), 0)

    for way in range(2):
        for chunk in range(CHUNKS):
            hop(way, far - 2, chunk).wait_send()
            if (chunk < CHUNKS // 2) == (way == 0):
                hop(way, far - 1, chunk).wait_send()

    def told(block, carry):
        @pl.when(lax.rem(z - block, STRIDE) == 0)
        def _():
            each_relay(block, lambda copy: copy.wait_send())

        return carry

    lax.fori_loop(0, z + 1, told, 0)

    def reached(target, carry):
        direct(target).wait_send()
        return carry

    lax.fori_loop(0, z, reached, 0)
    for k in range(2):
        weight_copy(k).wait_send()
    for way in range(2):
        for chunk in range(2):
            x_copy(way, 0, chunk, False).wait_send()
        x_copy(way, 1, way, False).wait_send()

    def sent(block, carry):
        @pl.when(lax.div(block, per_owner) != me)
        def _():
            owner_copy(block, *bias_way).wait_send()
            owner_copy(block, *part_way).wait_send()

        return carry

    lax.fori_loop(0, n_row, sent, 0)

    for slot in range(per_owner):
        total_f32 = None
        for giver in range(owners):
            pltpu.make_async_copy(
                stage.at[0], parts.at[giver, slot], part_recv.at[giver, slot]
            ).wait()
            part = parts[giver, slot].astype(jnp.float32)
            total_f32 = part if total_f32 is None else total_f32 + part
        for i in range(rows):
            tri[i, slot * rows : (slot + 1) * rows] = total_f32[i * rows : (i + 1) * rows]

    tri_normed = norm(tri[...].reshape(rows * half, width)).astype(jnp.bfloat16)
    second = first_ref[...].reshape(rows * half, width) + gate[...] * jnp.dot(
        tri_normed, mult_out_ref[...], preferred_element_type=jnp.float32
    )
    last_normed = norm(second).astype(jnp.bfloat16)
    hidden = jax.nn.relu(
        jnp.dot(last_normed, trans_up_ref[...], preferred_element_type=jnp.float32)
    ).astype(jnp.bfloat16)
    result = second + jnp.dot(hidden, trans_down_ref[...], preferred_element_type=jnp.float32)
    out_ref[...] = result.astype(jnp.bfloat16).reshape(rows, half, width)


def local(
    pair,
    length,
    chain,
    att_proj,
    att_bias,
    chain_bias,
    att_out,
    mult_in,
    mult_gate,
    mult_out,
    trans_up,
    trans_down,
):
    rows, cols, width = pair.shape
    n_row, n_col, n_sub = (lax.axis_size(a) for a in ("row", "col", "sub"))
    owners = n_col * n_sub
    per_owner = n_row // owners
    half = cols // n_sub
    total = rows * n_row
    heads_here = att_bias.shape[1]
    heads = heads_here * n_sub
    spread = att_out.shape[0]
    vmem = pl.BlockSpec(memory_space=pltpu.VMEM)
    smem = pl.BlockSpec(memory_space=pltpu.SMEM)
    dma = pltpu.SemaphoreType.DMA
    bf16, f32 = jnp.bfloat16, jnp.float32
    return pl.pallas_call(
        functools.partial(pair_kernel, n_row, n_col, n_sub),
        out_shape=jax.ShapeDtypeStruct((rows, half, width), bf16),
        in_specs=[smem] * 3 + [vmem] * 10,
        out_specs=vmem,
        scratch_shapes=[
            pltpu.VMEM((n_col, rows, cols, width), bf16),
            pltpu.VMEM((rows, total, 2 * width), bf16),
            pltpu.VMEM((rows, heads * half, width), bf16),
            pltpu.VMEM((rows, half, width), f32),
            pltpu.VMEM((rows, heads * half, total), f32),
            pltpu.VMEM((heads * half, total), f32),
            pltpu.VMEM((n_row, heads_here * rows, width), f32),
            pltpu.VMEM((owners, per_owner, heads_here * rows, width), f32),
            pltpu.VMEM((n_sub, 4, spread, width), bf16),
            pltpu.VMEM((n_sub, spread, width), bf16),
            pltpu.VMEM((rows, half, width), bf16),
            pltpu.VMEM((rows, half, width), f32),
            pltpu.VMEM((n_row, rows, half, width), bf16),
            pltpu.VMEM((rows, half, width), f32),
            pltpu.VMEM((2, rows * rows, width), f32),
            pltpu.VMEM((n_row, rows * rows, width), bf16),
            pltpu.VMEM((owners, per_owner, rows * rows, width), bf16),
            pltpu.VMEM((rows, half, width), f32),
            pltpu.VMEM((rows * half, width), f32),
            dma((2, 2, 2)),
            dma((2, 2, 2)),
            dma((2,)),
            dma((2,)),
            dma((n_row // STRIDE, STRIDE)),
            dma((n_row,)),
            dma((n_row,)),
            dma((n_row,)),
            dma((owners, per_owner)),
            dma((2, 2, CHUNKS)),
            dma((2, n_row // 2, CHUNKS)),
            dma((n_row,)),
            dma((owners, per_owner)),
        ],
        compiler_params=pltpu.CompilerParams(collective_id=0, has_side_effects=True),
    )(
        length,
        chain,
        chain_bias,
        pair,
        chain,
        att_bias.T,
        att_proj.transpose(1, 2, 0),
        att_out,
        mult_in,
        mult_gate,
        mult_out,
        trans_up,
        trans_down,
    )


def solution(mesh):
    placed = (
        P(("grp", "row"), "col", None),
        P("grp"),
        P("grp"),
        P(None, None, "sub"),
        P(None, "sub"),
        P("sub"),
        P("sub", None),
        P(),
        P(),
        P(),
        P(),
        P(),
    )
    return jax.shard_map(
        local,
        mesh=mesh,
        in_specs=placed,
        out_specs=P(("grp", "row"), ("col", "sub"), None),
        check_vma=False,
    )
```

```python
import functools

import jax
import jax.numpy as jnp
from jax import lax
from jax.experimental import pallas as pl
from jax.experimental.pallas import tpu as pltpu
from jax.sharding import PartitionSpec as P

MESH = pl.DeviceIdType.MESH
LAG = 3
STRIDE = 4


def norm(value):
    mean = jnp.mean(value, axis=-1, keepdims=True)
    centred = value - mean
    variance = jnp.mean(centred * centred, axis=-1, keepdims=True)
    return centred * lax.rsqrt(variance + 1e-05)


def pair_kernel(
    n_row,
    n_col,
    n_sub,
    length_ref,
    chain_ref,
    chain_bias_ref,
    pair_ref,
    chain_lanes_ref,
    att_bias_ref,
    att_w_ref,
    att_out_ref,
    mult_in_ref,
    mult_gate_ref,
    mult_out_ref,
    trans_up_ref,
    trans_down_ref,
    out_ref,
    raws,
    tile_f32,
    mine,
    kept,
    query_f32,
    query_rows,
    att_gate,
    scores,
    bias,
    pieces,
    bias_in,
    both_w,
    both_out,
    att_f32,
    first,
    first_in,
    whole_first,
    gathered,
    left,
    right_f32,
    stage_f32,
    stage,
    parts,
    tri,
    x_send,
    x_recv,
    weight_send,
    weight_recv,
    chain_send,
    chain_recv,
    bias_send,
    bias_recv,
    first_send,
    first_recv,
    ring_send,
    ring_recv,
    part_send,
    part_recv,
):
    rows, cols, width = pair_ref.shape
    half = cols // n_sub
    total = rows * n_row
    block_rows = rows // 2
    area = rows * rows
    heads_here = pieces.shape[1] // rows
    heads = heads_here * n_sub
    head_dim = width // heads
    group = heads * rows
    z = lax.axis_index("row")
    x = lax.axis_index("col")
    core = lax.axis_index("sub")
    owners = n_col * n_sub
    me = x * n_sub + core
    slots = n_row // owners
    far = n_row // 2
    up = lax.rem(z + 1, n_row)
    down = lax.rem(z + n_row - 1, n_row)
    length = length_ref[0]

    def row_at(offset):
        return lax.rem(z + (offset + n_row), n_row)

    def seat(owner):
        return {"col": lax.div(owner, n_sub), "sub": lax.rem(owner, n_sub)}

    barrier = pltpu.get_barrier_semaphore()
    for offset in (STRIDE, -STRIDE):
        pl.semaphore_signal(
            barrier, inc=1, device_id={"row": row_at(offset)}, device_id_type=MESH
        )
    for step in range(1, owners):
        pl.semaphore_signal(
            barrier, inc=1, device_id=seat(lax.rem(me + step, owners)), device_id_type=MESH
        )

    gang, rank = lax.div(z, STRIDE), lax.rem(z, STRIDE)

    def mate(n):
        return gang * STRIDE + lax.rem(rank + n, STRIDE)

    def greet(owner, carry):
        for n in range(1, STRIDE):
            pl.semaphore_signal(
                barrier, inc=1, device_id={"row": mate(n), **seat(owner)}, device_id_type=MESH
            )
        return carry

    lax.fori_loop(0, owners, greet, 0)
    for edge, neighbour in ((0, down), (STRIDE - 1, up)):

        @pl.when(rank == edge)
        def _():
            pl.semaphore_signal(
                barrier, inc=1, device_id={"row": neighbour}, device_id_type=MESH
            )

    raws[x] = pair_ref[...]
    both_out[core] = att_out_ref[...]
    both_w[core] = att_w_ref[...]
    right_f32[...] = jnp.zeros_like(right_f32)

    lane = lax.broadcasted_iota(jnp.int32, (1, width), 1)
    begin = x * cols
    turn = lax.rem(begin, width)
    key = begin + lax.rem(lane + (width - turn), width)
    key_chain = jnp.zeros((1, width), jnp.int32)
    for k in range(total // width):
        held = chain_lanes_ref[k * width : (k + 1) * width].reshape(1, width)
        key_chain = jnp.where(key // width == k, held, key_chain)
    key_bias = ((key < length).astype(jnp.float32) - 1.0) * 1000000000.0
    padding = jnp.zeros((width - cols, width), jnp.bfloat16)
    bias_w = att_bias_ref[...]
    for i in range(rows):
        keys_i = norm(pair_ref[i].astype(jnp.float32)).astype(jnp.bfloat16)
        keys_i = jnp.concatenate([keys_i, padding], axis=0)
        term = lax.dot_general(
            bias_w, keys_i, (((1,), (1,)), ((), ())), preferred_element_type=jnp.float32
        )
        term = pltpu.roll(term, turn, 1)
        same = (key_chain == chain_ref[z * rows + i]).astype(jnp.float32)
        for h in range(heads_here):
            at = h * rows + i
            pieces[z, at : at + 1] = term[h : h + 1] + chain_bias_ref[h] * same + key_bias

    at_edge = jnp.where(jnp.logical_or(rank == 0, rank == STRIDE - 1), 1, 0)
    pl.semaphore_wait(barrier, 2 + owners - 1 + (STRIDE - 1) * owners + at_edge)

    def weight_copy(k):
        source, target = [
            (att_w_ref, both_w.at[core]),
            (att_out_ref, both_out.at[core]),
        ][k]
        return pltpu.make_async_remote_copy(
            src_ref=source,
            dst_ref=target,
            send_sem=weight_send.at[k],
            recv_sem=weight_recv.at[k],
            device_id={"sub": 1 - core},
            device_id_type=MESH,
        )

    def x_copy(way, step, chunk, arrives):
        distance = step + 1 if arrives else step
        source = lax.rem(x + (n_col - distance if way == 0 else distance), n_col)
        block = raws.at[source, pl.ds(chunk * block_rows, block_rows)]
        return pltpu.make_async_remote_copy(
            src_ref=block,
            dst_ref=block,
            send_sem=x_send.at[way, step, chunk],
            recv_sem=x_recv.at[way, step, chunk],
            device_id={"col": lax.rem(x + (1 if way == 0 else n_col - 1), n_col)},
            device_id_type=MESH,
        )

    def bias_hop(block, offset, send_sem):
        return pltpu.make_async_remote_copy(
            src_ref=pieces.at[block],
            dst_ref=pieces.at[block],
            send_sem=send_sem,
            recv_sem=chain_recv.at[block],
            device_id={"row": row_at(offset)},
            device_id_type=MESH,
        )

    def bias_copy(block, stop, n):
        owner, slot = lax.rem(block, owners), lax.div(block, owners)
        return pltpu.make_async_remote_copy(
            src_ref=pieces.at[block],
            dst_ref=bias_in.at[me, slot],
            send_sem=bias_send.at[stop, n],
            recv_sem=bias_recv.at[me, slot],
            device_id={"row": mate(n), **seat(owner)},
            device_id_type=MESH,
        )

    def deliver(block, stop):
        slot = lax.div(block, owners)
        own = lax.rem(block, owners) == me
        for n in range(1, STRIDE):
            bias_copy(block, stop, n).start()

        @pl.when(own)
        def _():
            pltpu.make_async_copy(
                pieces.at[block], bias_in.at[me, slot], bias_recv.at[me, slot]
            ).start()

        @pl.when(jnp.logical_not(own))
        def _():
            bias_copy(block, stop, 0).start()

    gangs = n_row // STRIDE
    reach = gangs // 2
    nearer_downs = jnp.minimum(gangs - 1 - gang, reach)

    def turn_of(position):
        is_down = jnp.logical_and(position >= gang, position < gang + nearer_downs)
        hops = jnp.where(
            position < gang,
            position + 1,
            jnp.where(is_down, position - gang + 1, position - nearer_downs + 1),
        )
        origin = lax.rem(gang + gangs + jnp.where(is_down, hops, -hops), gangs)
        downs = jnp.minimum(origin, reach)
        goes_down = jnp.logical_and(is_down, hops < downs)
        goes_up = jnp.logical_and(jnp.logical_not(is_down), hops < gangs - 1 - downs)
        return origin * STRIDE + rank, goes_up, goes_down

    def pass_on(position, carry):
        block, goes_up, goes_down = turn_of(position)
        bias_hop(block, 0, chain_send.at[0, 0]).wait_recv()

        @pl.when(goes_up)
        def _():
            bias_hop(block, STRIDE, chain_send.at[position + 1, 0]).start()

        @pl.when(goes_down)
        def _():
            bias_hop(block, -STRIDE, chain_send.at[position + 1, 0]).start()

        deliver(block, position + 1)
        return carry

    def w_of(g):
        return jnp.concatenate([both_w[k, g] for k in range(n_sub)], axis=0)

    def times(value, weight):
        return lax.dot_general(
            value, weight, (((1,), (1,)), ((), ())), preferred_element_type=jnp.float32
        )

    def project(source, chunk):
        tile = raws[source, pl.ds(chunk * block_rows, block_rows)].astype(jnp.float32)
        tile_f32[...] = tile
        flat = norm(tile).astype(jnp.bfloat16).reshape(block_rows * cols, width)
        made = times(flat, w_kept).astype(jnp.bfloat16)
        kept[
            pl.ds(chunk * block_rows, block_rows), pl.ds(pl.multiple_of(source * cols, 32), cols)
        ] = made.reshape(block_rows, cols, 2 * width)
        for i in range(block_rows):
            mine[source, pl.ds(chunk * block_rows + i, rows, stride=rows)] = tile_f32[
                i, pl.ds(me * rows, rows)
            ]

    bias_hop(z, STRIDE, chain_send.at[0, 0]).start()

    @pl.when(gang > 0)
    def _():
        bias_hop(z, -STRIDE, chain_send.at[0, 1]).start()

    deliver(z, 0)
    for k in range(2):
        weight_copy(k).start()
    for chunk in range(2):
        for way in range(2):
            x_copy(way, 0, chunk if way == 0 else 1 - chunk, False).start()

    lax.fori_loop(0, gang, pass_on, 0)
    for k in range(2):
        weight_copy(k).wait_recv()
    w_query, w_gate = w_of(0), w_of(3)
    w_kept = jnp.concatenate([w_of(1), w_of(2)], axis=0)
    for chunk in range(2):
        project(x, chunk)

    x_up = lax.rem(x + n_col - 1, n_col)
    x_down = lax.rem(x + 1, n_col)
    x_far = lax.rem(x + 2, n_col)
    x_copy(0, 0, 0, True).wait_recv()
    x_copy(0, 1, 0, False).start()
    x_copy(1, 0, 1, True).wait_recv()
    x_copy(1, 1, 1, False).start()
    project(x_up, 0)
    project(x_down, 1)
    x_copy(0, 0, 1, True).wait_recv()
    project(x_up, 1)
    x_copy(1, 0, 0, True).wait_recv()
    project(x_down, 0)
    x_copy(0, 1, 0, True).wait_recv()
    project(x_far, 0)
    x_copy(1, 1, 1, True).wait_recv()
    project(x_far, 1)

    lane_head = lax.broadcasted_iota(jnp.int32, (rows, width), 1) // head_dim
    for q in range(slots):
        tile = norm(mine[q]).astype(jnp.bfloat16)
        query_f32[q] = (
            (times(tile, w_query) * head_dim ** (-0.5)).astype(jnp.bfloat16).astype(jnp.float32)
        )
        att_gate[q] = jax.nn.sigmoid(times(tile, w_gate))

    def score(i, carry):
        for q in range(slots):
            line = query_f32[q, pl.ds(i, rows, stride=rows)]
            for h in range(heads):
                at = q * group + h * rows
                query_rows[at : at + rows] = jnp.where(lane_head == h, line, 0.0)
        scores[i] = times(query_rows[...].astype(jnp.bfloat16), kept[i, :, :width])
        return carry

    lax.fori_loop(0, rows, score, 0)
    later = jnp.where(
        gang == reach - 2, 2, jnp.where((gang == 0) | (gang > reach), 0, 1)
    )
    ready = gangs - 1 - later
    lax.fori_loop(gang, ready, pass_on, 0)

    def source(way, step):
        return lax.rem(z + (n_row - step if way == 0 else step), n_row)

    def ring_copy(way, step, chunk, arrives):
        block = gathered.at[source(way, step), chunk]
        return pltpu.make_async_remote_copy(
            src_ref=block,
            dst_ref=block,
            send_sem=ring_send.at[way, lax.rem(step, 2), chunk],
            recv_sem=ring_recv.at[way, step - 1 if arrives else step, chunk],
            device_id={"row": up if way == 0 else down},
            device_id_type=MESH,
        )

    def hop(way, step, chunk):
        return ring_copy(way, step, chunk, False)

    def arrival(way, step, chunk):
        return ring_copy(way, step, chunk, True)

    def part_copy(block):
        dest, slot = lax.div(block, slots), lax.rem(block, slots)
        return pltpu.make_async_remote_copy(
            src_ref=stage.at[block],
            dst_ref=parts.at[me, slot],
            send_sem=part_send.at[block],
            recv_sem=part_recv.at[me, slot],
            device_id=seat(dest),
            device_id_type=MESH,
        )

    def give(block):
        slot = lax.rem(block, slots)
        own = lax.div(block, slots) == me
        stage[block] = stage_f32[block].astype(jnp.bfloat16)

        @pl.when(own)
        def _():
            pltpu.make_async_copy(
                stage.at[block], parts.at[me, slot], part_recv.at[me, slot]
            ).start()

        @pl.when(jnp.logical_not(own))
        def _():
            part_copy(block).start()

    def first_copy(q):
        block = q * owners + me
        dest, slot = lax.div(block, slots), lax.rem(block, slots)
        return pltpu.make_async_remote_copy(
            src_ref=first.at[q],
            dst_ref=first_in.at[slot],
            send_sem=first_send.at[q],
            recv_sem=first_recv.at[slot],
            device_id=seat(dest),
            device_id_type=MESH,
        )

    def first_stays(q):
        return lax.div(q * owners + me, slots) == me

    def multiply(block, q):
        right_f32[:area] = gathered[block, q].astype(jnp.float32)
        for i in range(rows):
            total_i = None
            for k in range(rows):
                term = left[q, k * rows + i : k * rows + i + 1] * right_f32[
                    k * rows : k * rows + 16
                ]
                total_i = term if total_i is None else total_i + term
            stage_f32[block, i * rows : (i + 1) * rows] += total_i[:rows]

    def settle(low, high):
        for q in range(low, high):
            for giver in range(owners):
                pltpu.make_async_copy(
                    pieces.at[0], bias_in.at[giver, q], bias_recv.at[giver, q]
                ).wait()
            for h in range(heads):
                giver, own_head = h // heads_here, h % heads_here
                at = q * group + h * rows
                for k in range(total // width):
                    line = None
                    for tile in range(n_col):
                        start = tile * cols - k * width
                        if start + cols <= 0 or start >= width:
                            continue
                        held = bias_in[
                            tile * n_sub + giver, q, own_head * rows : (own_head + 1) * rows
                        ]
                        line = held if line is None else jnp.where(lane_of >= start, held, line)
                    bias[at : at + rows, k * width : (k + 1) * width] = line

        def attend(i, carry):
            logits = scores[i, low * group : high * group] + bias[low * group : high * group]
            weights = jnp.exp(logits - jnp.max(logits, axis=-1, keepdims=True))
            weights = weights * (1.0 / jnp.sum(weights, axis=-1, keepdims=True))
            made = jnp.dot(
                weights.astype(jnp.bfloat16), kept[i, :, width:], preferred_element_type=jnp.float32
            )
            for q in range(low, high):
                at = (q - low) * group
                taken = made[at : at + rows]
                for h in range(1, heads):
                    other = made[at + h * rows : at + (h + 1) * rows]
                    taken = jnp.where(lane_head == h, other, taken)
                att_f32[q, pl.ds(i, rows, stride=rows)] = taken
            return carry

        lax.fori_loop(0, rows, attend, 0, unroll=2)
        for q in range(low, high):
            attended = (att_f32[q] * att_gate[q]).astype(jnp.bfloat16)
            first_q = mine[q] + jnp.dot(
                attended,
                both_out[...].reshape(width, width),
                preferred_element_type=jnp.float32,
            )
            first[q] = first_q
            quad = jnp.dot(
                norm(first_q).astype(jnp.bfloat16),
                mult_in_ref[...],
                preferred_element_type=jnp.float32,
            )
            index = lax.broadcasted_iota(jnp.int32, (area, width), 0)
            here_row = z * rows + lax.rem(index, rows)
            here_col = (q * owners + me) * rows + lax.div(index, rows)
            valid = ((here_row < length) & (here_col < length)).astype(jnp.float32)
            a, b, c, d = [quad[:, k * width : (k + 1) * width] for k in range(4)]
            left[q] = (valid * jax.nn.sigmoid(b) * a).astype(jnp.bfloat16).astype(jnp.float32)
            gathered[z, q] = (valid * jax.nn.sigmoid(d) * c).astype(jnp.bfloat16)
            for way in range(2):
                hop(way, 0, q).start()
        for q in range(low, high):
            slot = lax.rem(q * owners + me, slots)

            @pl.when(first_stays(q))
            def _():
                pltpu.make_async_copy(first.at[q], first_in.at[slot], first_recv.at[slot]).start()

            @pl.when(jnp.logical_not(first_stays(q)))
            def _():
                first_copy(q).start()

        def own(q, carry):
            multiply(z, q)
            return carry

        lax.fori_loop(low, high, own, 0)

    def visit(step, chunk):
        is_last = [chunk < slots // 2, chunk >= slots // 2]
        present = [
            jnp.logical_or(step < far, jnp.logical_and(step == far, last)) for last in is_last
        ]
        for way in range(2):
            goes = jnp.logical_or(
                step < far - 1, jnp.logical_and(step == far - 1, is_last[way])
            )

            @pl.when(present[way])
            def _():
                arrival(way, step, chunk).wait_recv()

            @pl.when(jnp.logical_and(goes, step >= 2))
            def _():
                hop(way, step, chunk).wait_send()

            @pl.when(goes)
            def _():
                hop(way, step, chunk).start()

        for way in range(2):

            @pl.when(present[way])
            def _():
                block = source(way, step)
                multiply(block, chunk)

                @pl.when(chunk == slots - 1)
                def _():
                    give(block)

    lane_of = lax.broadcasted_iota(jnp.int32, (rows, width), 1)
    stage_f32[...] = jnp.zeros_like(stage_f32)
    early = slots - 1
    settle(0, early)

    late_step = jnp.where(gang == reach - 1, LAG, 1)

    def early_step(step, carry):
        def early_visit(chunk, inner):
            visit(step, chunk)
            return inner

        lax.fori_loop(0, early, early_visit, 0)
        lax.fori_loop(jnp.where(step == late_step, ready, gangs - 1), gangs - 1, pass_on, 0)
        return carry

    lax.fori_loop(1, LAG + 1, early_step, 0)
    settle(early, slots)
    give(z)

    def both_visit(n, carry):
        chunk = lax.rem(n, slots)
        step = LAG + 1 + lax.div(n, slots) - jnp.where(chunk == early, LAG, 0)
        visit(step, chunk)
        return carry

    lax.fori_loop(0, far * slots, both_visit, 0)

    for way in range(2):
        for chunk in range(slots):
            last = far - 1 if (chunk < slots // 2) == (way == 0) else far - 2
            hop(way, last - 1, chunk).wait_send()
            hop(way, last, chunk).wait_send()

    def told(position, carry):
        block, goes_up, goes_down = turn_of(position)

        @pl.when(jnp.logical_or(goes_up, goes_down))
        def _():
            bias_hop(block, STRIDE, chain_send.at[position + 1, 0]).wait_send()

        return carry

    lax.fori_loop(0, gangs - 1, told, 0)
    bias_hop(z, STRIDE, chain_send.at[0, 0]).wait_send()

    @pl.when(gang > 0)
    def _():
        bias_hop(z, -STRIDE, chain_send.at[0, 1]).wait_send()

    def delivered(stop, carry):
        block = jnp.where(stop == 0, z, turn_of(jnp.maximum(stop - 1, 0))[0])
        for n in range(1, STRIDE):
            bias_copy(block, stop, n).wait_send()

        @pl.when(lax.rem(block, owners) != me)
        def _():
            bias_copy(block, stop, 0).wait_send()

        return carry

    lax.fori_loop(0, gangs, delivered, 0)
    for k in range(2):
        weight_copy(k).wait_send()
    for way in range(2):
        for chunk in range(2):
            x_copy(way, 0, chunk, False).wait_send()
        x_copy(way, 1, way, False).wait_send()
    for q in range(slots):

        @pl.when(jnp.logical_not(first_stays(q)))
        def _():
            first_copy(q).wait_send()

    def sent(block, carry):
        @pl.when(lax.div(block, slots) != me)
        def _():
            part_copy(block).wait_send()

        return carry

    lax.fori_loop(0, n_row, sent, 0)

    for slot in range(slots):
        pltpu.make_async_copy(first.at[0], first_in.at[slot], first_recv.at[slot]).wait()
        sum_f32 = None
        for giver in range(owners):
            pltpu.make_async_copy(
                stage.at[0], parts.at[giver, slot], part_recv.at[giver, slot]
            ).wait()
            part = parts[giver, slot].astype(jnp.float32)
            sum_f32 = part if sum_f32 is None else sum_f32 + part
        for i in range(rows):
            tri[i, slot * rows : (slot + 1) * rows] = sum_f32[i * rows : (i + 1) * rows]
            whole_first[i, slot * rows : (slot + 1) * rows] = first_in[
                slot, pl.ds(i, rows, stride=rows)
            ]

    first_all = whole_first[...].reshape(rows * half, width)
    gate = jax.nn.sigmoid(
        jnp.dot(
            norm(first_all).astype(jnp.bfloat16),
            mult_gate_ref[...],
            preferred_element_type=jnp.float32,
        )
    )
    tri_normed = norm(tri[...].reshape(rows * half, width)).astype(jnp.bfloat16)
    second = first_all + gate * jnp.dot(
        tri_normed, mult_out_ref[...], preferred_element_type=jnp.float32
    )
    last_normed = norm(second).astype(jnp.bfloat16)
    hidden = jax.nn.relu(
        jnp.dot(last_normed, trans_up_ref[...], preferred_element_type=jnp.float32)
    ).astype(jnp.bfloat16)
    result = second + jnp.dot(hidden, trans_down_ref[...], preferred_element_type=jnp.float32)
    out_ref[...] = result.astype(jnp.bfloat16).reshape(rows, half, width)


def local(
    pair,
    length,
    chain,
    att_proj,
    att_bias,
    chain_bias,
    att_out,
    mult_in,
    mult_gate,
    mult_out,
    trans_up,
    trans_down,
):
    rows, cols, width = pair.shape
    n_row, n_col, n_sub = (lax.axis_size(a) for a in ("row", "col", "sub"))
    owners = n_col * n_sub
    slots = n_row // owners
    area = rows * rows
    half = cols // n_sub
    total = rows * n_row
    heads_here = att_bias.shape[1]
    heads = heads_here * n_sub
    spread = att_out.shape[0]
    vmem = pl.BlockSpec(memory_space=pltpu.VMEM)
    smem = pl.BlockSpec(memory_space=pltpu.SMEM)
    dma = pltpu.SemaphoreType.DMA
    bf16, f32 = jnp.bfloat16, jnp.float32
    return pl.pallas_call(
        functools.partial(pair_kernel, n_row, n_col, n_sub),
        out_shape=jax.ShapeDtypeStruct((rows, half, width), bf16),
        in_specs=[smem] * 3 + [vmem] * 10,
        out_specs=vmem,
        scratch_shapes=[
            pltpu.VMEM((n_col, rows, cols, width), bf16),
            pltpu.VMEM((rows // 2, cols, width), f32),
            pltpu.VMEM((slots, area, width), f32),
            pltpu.VMEM((rows, total, 2 * width), bf16),
            pltpu.VMEM((slots, area, width), f32),
            pltpu.VMEM((heads * half, width), f32),
            pltpu.VMEM((slots, area, width), f32),
            pltpu.VMEM((rows, heads * half, total), f32),
            pltpu.VMEM((heads * half, total), f32),
            pltpu.VMEM((n_row, heads_here * rows, width), f32),
            pltpu.VMEM((owners, slots, heads_here * rows, width), f32),
            pltpu.VMEM((n_sub, 4, spread, width), bf16),
            pltpu.VMEM((n_sub, spread, width), bf16),
            pltpu.VMEM((slots, area, width), f32),
            pltpu.VMEM((slots, area, width), f32),
            pltpu.VMEM((slots, area, width), f32),
            pltpu.VMEM((rows, half, width), f32),
            pltpu.VMEM((n_row, slots, area, width), bf16),
            pltpu.VMEM((slots, area, width), f32),
            pltpu.VMEM((area + 8, width), f32),
            pltpu.VMEM((n_row, area, width), f32),
            pltpu.VMEM((n_row, area, width), bf16),
            pltpu.VMEM((owners, slots, area, width), bf16),
            pltpu.VMEM((rows, half, width), f32),
            dma((2, 2, 2)),
            dma((2, 2, 2)),
            dma((2,)),
            dma((2,)),
            dma((n_row // STRIDE, 2)),
            dma((n_row,)),
            dma((n_row // STRIDE, STRIDE)),
            dma((owners, slots)),
            dma((slots,)),
            dma((slots,)),
            dma((2, 2, slots)),
            dma((2, n_row // 2, slots)),
            dma((n_row,)),
            dma((owners, slots)),
        ],
        compiler_params=pltpu.CompilerParams(collective_id=0, has_side_effects=True),
    )(
        length,
        chain,
        chain_bias,
        pair,
        chain,
        att_bias.T,
        att_proj.transpose(1, 2, 0),
        att_out,
        mult_in,
        mult_gate,
        mult_out,
        trans_up,
        trans_down,
    )


def solution(mesh):
    placed = (
        P(("grp", "row"), "col", None),
        P("grp"),
        P("grp"),
        P(None, None, "sub"),
        P(None, "sub"),
        P("sub"),
        P("sub", None),
        P(),
        P(),
        P(),
        P(),
        P(),
    )
    return jax.shard_map(
        local,
        mesh=mesh,
        in_specs=placed,
        out_specs=P(("grp", "row"), ("col", "sub"), None),
        check_vma=False,
    )
```

```python
import functools

import jax
import jax.numpy as jnp
from jax import lax
from jax.experimental import pallas as pl
from jax.experimental.pallas import tpu as pltpu
from jax.sharding import PartitionSpec as P

MESH = pl.DeviceIdType.MESH
CHUNKS = 4
STRIDE = 4
LOCAL = (-1, 1, 2)


def norm(value):
    mean = jnp.mean(value, axis=-1, keepdims=True)
    centred = value - mean
    variance = jnp.mean(centred * centred, axis=-1, keepdims=True)
    return centred * lax.rsqrt(variance + 1e-05)


def pair_kernel(
    n_row,
    n_col,
    n_sub,
    length_ref,
    chain_ref,
    chain_bias_ref,
    pair_ref,
    chain_lanes_ref,
    att_bias_ref,
    att_w_ref,
    att_out_ref,
    mult_in_ref,
    mult_gate_ref,
    mult_out_ref,
    trans_up_ref,
    trans_down_ref,
    out_ref,
    normed,
    kept,
    queries,
    att_gate,
    scores,
    bias,
    pieces,
    bias_in,
    both_w,
    both_out,
    attended,
    first_ref,
    gathered,
    left,
    stage_f32,
    stage,
    parts,
    tri,
    gate,
    x_send,
    x_recv,
    swap_send,
    swap_recv,
    weight_send,
    weight_recv,
    chain_send,
    chain_recv,
    bias_send,
    bias_recv,
    ring_send,
    ring_recv,
    part_send,
    part_recv,
):
    rows, cols, width = pair_ref.shape
    half = cols // n_sub
    total = rows * n_row
    piece = rows // CHUNKS
    block_rows = rows // 2
    heads_here = pieces.shape[1] // rows
    heads = heads_here * n_sub
    head_dim = width // heads
    z = lax.axis_index("row")
    x = lax.axis_index("col")
    core = lax.axis_index("sub")
    owners = n_col * n_sub
    me = x * n_sub + core
    per_owner = n_row // owners
    far = n_row // 2
    up = lax.rem(z + 1, n_row)
    down = lax.rem(z + n_row - 1, n_row)
    length = length_ref[0]

    def row_at(offset):
        return lax.rem(z + (offset + n_row), n_row)

    barrier = pltpu.get_barrier_semaphore()
    near = (1, -1, 2, -2, STRIDE, -STRIDE)
    for offset in near:
        pl.semaphore_signal(
            barrier, inc=1, device_id={"row": row_at(offset)}, device_id_type=MESH
        )
    for step in range(1, owners):
        other = lax.rem(me + step, owners)
        pl.semaphore_signal(
            barrier,
            inc=1,
            device_id={"col": lax.div(other, n_sub), "sub": lax.rem(other, n_sub)},
            device_id_type=MESH,
        )

    normed[x] = norm(pair_ref[...].astype(jnp.float32)).astype(jnp.bfloat16)
    both_out[core] = att_out_ref[...]
    both_w[core] = att_w_ref[...]

    lane = lax.broadcasted_iota(jnp.int32, (1, width), 1)
    begin = x * cols
    turn = lax.rem(begin, width)
    key = begin + lax.rem(lane + (width - turn), width)
    key_chain = jnp.zeros((1, width), jnp.int32)
    for k in range(total // width):
        held = chain_lanes_ref[k * width : (k + 1) * width].reshape(1, width)
        key_chain = jnp.where(key // width == k, held, key_chain)
    key_bias = ((key < length).astype(jnp.float32) - 1.0) * 1000000000.0
    padding = jnp.zeros((width - cols, width), jnp.bfloat16)
    bias_w = att_bias_ref[...]
    for i in range(rows):
        keys_i = jnp.concatenate([normed[x, i], padding], axis=0)
        term = lax.dot_general(
            bias_w, keys_i, (((1,), (1,)), ((), ())), preferred_element_type=jnp.float32
        )
        term = pltpu.roll(term, turn, 1)
        same = (key_chain == chain_ref[z * rows + i]).astype(jnp.float32)
        for h in range(heads_here):
            at = h * rows + i
            pieces[z, at : at + 1] = term[h : h + 1] + chain_bias_ref[h] * same + key_bias

    pl.semaphore_wait(barrier, len(near) + owners - 1)

    def weight_copy(k):
        source, target = [
            (att_w_ref, both_w.at[core]),
            (att_out_ref, both_out.at[core]),
        ][k]
        return pltpu.make_async_remote_copy(
            src_ref=source,
            dst_ref=target,
            send_sem=weight_send.at[k],
            recv_sem=weight_recv.at[k],
            device_id={"sub": 1 - core},
            device_id_type=MESH,
        )

    quarter = block_rows // 2
    x_up = lax.rem(x + n_col - 1, n_col)
    x_down = lax.rem(x + 1, n_col)
    x_far = lax.rem(x + 2, n_col)

    def x_copy(way, step, arrives):
        distance = step + 1 if arrives else step
        source = lax.rem(x + (n_col - distance if way == 0 else distance), n_col)
        begin_row = core * block_rows + (quarter if step == 1 and way == 1 else 0)
        block = normed.at[source, pl.ds(begin_row, block_rows if step == 0 else quarter)]
        return pltpu.make_async_remote_copy(
            src_ref=block,
            dst_ref=block,
            send_sem=x_send.at[way, step],
            recv_sem=x_recv.at[way, step],
            device_id={"col": lax.rem(x + (1 if way == 0 else n_col - 1), n_col)},
            device_id_type=MESH,
        )

    def swap(k, holder):
        source = (x_up, x_down, x_far, x_far)[k]
        begin_row = holder * block_rows + (quarter if k == 3 else 0)
        block = normed.at[source, pl.ds(begin_row, block_rows if k < 2 else quarter)]
        return pltpu.make_async_remote_copy(
            src_ref=block,
            dst_ref=block,
            send_sem=swap_send.at[k],
            recv_sem=swap_recv.at[k],
            device_id={"sub": 1 - core},
            device_id_type=MESH,
        )

    def bias_hop(stop, k, block, offset):
        return pltpu.make_async_remote_copy(
            src_ref=pieces.at[block],
            dst_ref=pieces.at[block],
            send_sem=chain_send.at[stop, k],
            recv_sem=chain_recv.at[block],
            device_id={"row": row_at(offset)},
            device_id_type=MESH,
        )

    def owner_copy(block, source, target, send_sem, recv_sem):
        dest = lax.div(block, per_owner)
        return pltpu.make_async_remote_copy(
            src_ref=source.at[block],
            dst_ref=target.at[me, lax.rem(block, per_owner)],
            send_sem=send_sem.at[block],
            recv_sem=recv_sem.at[me, lax.rem(block, per_owner)],
            device_id={"col": lax.div(dest, n_sub), "sub": lax.rem(dest, n_sub)},
            device_id_type=MESH,
        )

    def to_owner(block, source, target, send_sem, recv_sem):
        slot = lax.rem(block, per_owner)
        mine = lax.div(block, per_owner) == me

        @pl.when(mine)
        def _():
            pltpu.make_async_copy(
                source.at[block], target.at[me, slot], recv_sem.at[me, slot]
            ).start()

        @pl.when(jnp.logical_not(mine))
        def _():
            owner_copy(block, source, target, send_sem, recv_sem).start()

    bias_way = (pieces, bias_in, bias_send, bias_recv)
    part_way = (stage, parts, part_send, part_recv)
    ups = n_row // (2 * STRIDE)

    def hops_of(stop):
        if stop == 0:
            ahead = [(0, STRIDE), (len(LOCAL) + 1, -STRIDE)]
        elif stop < ups:
            ahead = [(0, STRIDE)]
        elif stop == ups or stop == 2 * ups - 1:
            ahead = []
        else:
            ahead = [(0, -STRIDE)]
        return ahead + [(1 + n, offset) for n, offset in enumerate(LOCAL)]

    def block_of(stop):
        return row_at(-STRIDE * stop if stop <= ups else STRIDE * (stop - ups))

    def pass_on(stop):
        block = block_of(stop)
        if stop > 0:
            bias_hop(stop, 0, block, 0).wait_recv()
        for k, offset in hops_of(stop):
            bias_hop(stop, k, block, offset).start()
        to_owner(block, *bias_way)

    def take_local(stop):
        for offset in LOCAL:
            block = lax.rem(block_of(stop) + (n_row - offset), n_row)
            bias_hop(stop, 0, block, 0).wait_recv()
            to_owner(block, *bias_way)

    def project(source, chunk):
        tile = normed[source, pl.ds(chunk * block_rows, block_rows)]
        made = times(tile.reshape(block_rows * cols, width), w_kept).astype(jnp.bfloat16)
        kept[
            pl.ds(chunk * block_rows, block_rows), pl.ds(pl.multiple_of(source * cols, 32), cols)
        ] = made.reshape(block_rows, cols, 2 * width)

    def score(i, carry):
        scores[i] = lax.dot_general(
            queries[i],
            kept[i, :, :width],
            (((1,), (1,)), ((), ())),
            preferred_element_type=jnp.float32,
        )
        return carry

    for way in range(2):
        x_copy(way, 0, False).start()
    pass_on(0)
    for k in range(2):
        weight_copy(k).start()
    for k in range(2):
        weight_copy(k).wait_recv()

    def joined(g):
        return jnp.concatenate([both_w[k, g] for k in range(n_sub)], axis=0)

    def times(value, weight):
        return lax.dot_general(
            value, weight, (((1,), (1,)), ((), ())), preferred_element_type=jnp.float32
        )

    w_query, w_gate = joined(0), joined(3)
    w_kept = jnp.concatenate([joined(1), joined(2)], axis=0)
    tile = normed[x, :, pl.ds(pl.multiple_of(core * half, 16), half)].reshape(rows * half, width)
    query = (times(tile, w_query) * head_dim ** (-0.5)).astype(jnp.bfloat16)
    head_of = lax.broadcasted_iota(jnp.int32, (rows * half, width), 1) // head_dim
    for h in range(heads):
        queries[:, h * half : (h + 1) * half] = jnp.where(
            head_of == h, query, jnp.zeros_like(query)
        ).reshape(rows, half, width)
    att_gate[...] = jax.nn.sigmoid(times(tile, w_gate)).reshape(rows, half, width)
    for chunk in range(2):
        project(x, chunk)

    def stage_of(step):
        if step <= ups:
            pass_on(step)
        if step < ups:
            pass_on(ups + step)
        take_local(step - 1)
        if 1 <= step - 1 < ups:
            take_local(ups + step - 1)

    for way in range(2):
        x_copy(way, 0, True).wait_recv()
        x_copy(way, 1, False).start()
        swap(way, core).start()
    stage_of(1)
    project(x_up, core)
    project(x_down, core)
    for way in range(2):
        x_copy(way, 1, True).wait_recv()
        swap(2 + way, core).start()
    stage_of(2)
    project(x_far, core)
    swap(0, 1 - core).wait_recv()
    project(x_up, 1 - core)
    swap(1, 1 - core).wait_recv()
    project(x_down, 1 - core)
    stage_of(3)
    swap(2, 1 - core).wait_recv()
    swap(3, 1 - core).wait_recv()
    project(x_far, 1 - core)
    lax.fori_loop(0, block_rows, score, 0)
    stage_of(4)
    lax.fori_loop(block_rows, rows, score, 0)
    take_local(ups)

    for slot in range(per_owner):
        for giver in range(owners):
            pltpu.make_async_copy(
                pieces.at[0], bias_in.at[giver, slot], bias_recv.at[giver, slot]
            ).wait()
    lane = lax.broadcasted_iota(jnp.int32, (rows, width), 1)
    for slot in range(per_owner):
        for h in range(heads):
            giver, own_head = h // heads_here, h % heads_here
            held = [
                bias_in[k * n_sub + giver, slot, own_head * rows : (own_head + 1) * rows]
                for k in range(n_col)
            ]
            at = h * half + slot * rows
            for k in range(total // width):
                line = None
                for source in range(n_col):
                    begin = source * cols - k * width
                    if begin + cols <= 0 or begin >= width:
                        continue
                    line = held[source] if line is None else jnp.where(lane >= begin, held[source], line)
                bias[at : at + rows, k * width : (k + 1) * width] = line

    head_of = lax.broadcasted_iota(jnp.int32, (half, width), 1) // head_dim

    def attend(i, carry):
        logits = scores[i] + bias[...]
        weights = jnp.exp(logits - jnp.max(logits, axis=-1, keepdims=True))
        weights = weights * (1.0 / jnp.sum(weights, axis=-1, keepdims=True))
        mixed_values = jnp.dot(
            weights.astype(jnp.bfloat16), kept[i, :, width:], preferred_element_type=jnp.float32
        )
        taken = jnp.zeros((half, width), jnp.float32)
        for h in range(heads):
            taken = jnp.where(head_of == h, mixed_values[h * half : (h + 1) * half], taken)
        attended[i] = (taken * att_gate[i]).astype(jnp.bfloat16)
        return carry

    lax.fori_loop(0, rows, attend, 0, unroll=2)
    first_ref[...] = pair_ref[:, pl.ds(pl.multiple_of(core * half, 16), half)].astype(
        jnp.float32
    ) + jnp.dot(
        attended[...].reshape(rows * half, width),
        both_out[...].reshape(width, width),
        preferred_element_type=jnp.float32,
    ).reshape(rows, half, width)

    first = first_ref[...].reshape(rows * half, width)
    mixed = norm(first).astype(jnp.bfloat16)
    quad = jnp.dot(mixed, mult_in_ref[...], preferred_element_type=jnp.float32)
    shape = (rows, half, width)
    here_row = z * rows + lax.broadcasted_iota(jnp.int32, shape, 0)
    here_col = (x * n_sub + core) * half + lax.broadcasted_iota(jnp.int32, shape, 1)
    valid = ((here_row < length) & (here_col < length)).astype(jnp.float32)
    a, b, c, d = [quad[:, k * width : (k + 1) * width].reshape(shape) for k in range(4)]
    left[...] = (valid * jax.nn.sigmoid(b) * a).astype(jnp.bfloat16).astype(jnp.float32)
    gathered[z] = (valid * jax.nn.sigmoid(d) * c).astype(jnp.bfloat16)
    gate[...] = jax.nn.sigmoid(
        jnp.dot(mixed, mult_gate_ref[...], preferred_element_type=jnp.float32)
    )

    def source(way, step):
        return lax.rem(z + (n_row - step if way == 0 else step), n_row)

    def ring_copy(way, step, chunk, arrives):
        block = gathered.at[source(way, step), pl.ds(chunk * piece, piece)]
        return pltpu.make_async_remote_copy(
            src_ref=block,
            dst_ref=block,
            send_sem=ring_send.at[way, lax.rem(step, 2), chunk],
            recv_sem=ring_recv.at[way, step - 1 if arrives else step, chunk],
            device_id={"row": up if way == 0 else down},
            device_id_type=MESH,
        )

    def hop(way, step, chunk):
        return ring_copy(way, step, chunk, False)

    def arrival(way, step, chunk):
        return ring_copy(way, step, chunk, True)

    def multiply(owner, chunk, lane):
        for jj in range(piece):
            j = chunk * piece + jj
            right = gathered[owner, j].astype(jnp.float32)
            for i in range(rows):
                stage_f32[lane, pl.ds(i * rows + j, 1)] = jnp.sum(
                    left[i] * right, axis=0, keepdims=True
                )

    def give(block, lane):
        stage[block] = stage_f32[lane].astype(jnp.bfloat16)
        to_owner(block, *part_way)

    for chunk in range(CHUNKS):
        for way in range(2):
            hop(way, 0, chunk).start()

    def own(chunk, carry):
        multiply(z, chunk, 0)
        return carry

    lax.fori_loop(0, CHUNKS, own, 0)
    give(z, 0)

    def visit(n, carry):
        step = lax.div(n, CHUNKS) + 1
        chunk = lax.rem(n, CHUNKS)
        for way in range(2):
            arrival(way, step, chunk).wait_recv()
            last = chunk < CHUNKS // 2 if way == 0 else chunk >= CHUNKS // 2

            @pl.when(step >= 2)
            def _():
                hop(way, step, chunk).wait_send()

            @pl.when(jnp.logical_or(step < far - 1, last))
            def _():
                hop(way, step, chunk).start()

        for way in range(2):
            multiply(source(way, step), chunk, way)

        @pl.when(chunk == CHUNKS - 1)
        def _():
            for way in range(2):
                give(source(way, step), way)

        return carry

    lax.fori_loop(0, (far - 1) * CHUNKS, visit, 0)

    for chunk in range(CHUNKS):
        arrival(0 if chunk < CHUNKS // 2 else 1, far, chunk).wait_recv()
        multiply(source(0, far), chunk, 0)
    give(source(0, far), 0)

    for way in range(2):
        for chunk in range(CHUNKS):
            hop(way, far - 2, chunk).wait_send()
            if (chunk < CHUNKS // 2) == (way == 0):
                hop(way, far - 1, chunk).wait_send()

    for stop in range(2 * ups):
        for k, offset in hops_of(stop):
            bias_hop(stop, k, block_of(stop), offset).wait_send()
    for k in range(2):
        weight_copy(k).wait_send()
    for way in range(2):
        for step in range(2):
            x_copy(way, step, False).wait_send()
    for k in range(4):
        swap(k, core).wait_send()

    def sent(block, carry):
        @pl.when(lax.div(block, per_owner) != me)
        def _():
            owner_copy(block, *bias_way).wait_send()
            owner_copy(block, *part_way).wait_send()

        return carry

    lax.fori_loop(0, n_row, sent, 0)

    for slot in range(per_owner):
        total_f32 = None
        for giver in range(owners):
            pltpu.make_async_copy(
                stage.at[0], parts.at[giver, slot], part_recv.at[giver, slot]
            ).wait()
            part = parts[giver, slot].astype(jnp.float32)
            total_f32 = part if total_f32 is None else total_f32 + part
        for i in range(rows):
            tri[i, slot * rows : (slot + 1) * rows] = total_f32[i * rows : (i + 1) * rows]

    tri_normed = norm(tri[...].reshape(rows * half, width)).astype(jnp.bfloat16)
    second = first_ref[...].reshape(rows * half, width) + gate[...] * jnp.dot(
        tri_normed, mult_out_ref[...], preferred_element_type=jnp.float32
    )
    last_normed = norm(second).astype(jnp.bfloat16)
    hidden = jax.nn.relu(
        jnp.dot(last_normed, trans_up_ref[...], preferred_element_type=jnp.float32)
    ).astype(jnp.bfloat16)
    result = second + jnp.dot(hidden, trans_down_ref[...], preferred_element_type=jnp.float32)
    out_ref[...] = result.astype(jnp.bfloat16).reshape(rows, half, width)


def local(
    pair,
    length,
    chain,
    att_proj,
    att_bias,
    chain_bias,
    att_out,
    mult_in,
    mult_gate,
    mult_out,
    trans_up,
    trans_down,
):
    rows, cols, width = pair.shape
    n_row, n_col, n_sub = (lax.axis_size(a) for a in ("row", "col", "sub"))
    owners = n_col * n_sub
    per_owner = n_row // owners
    half = cols // n_sub
    total = rows * n_row
    heads_here = att_bias.shape[1]
    heads = heads_here * n_sub
    spread = att_out.shape[0]
    vmem = pl.BlockSpec(memory_space=pltpu.VMEM)
    smem = pl.BlockSpec(memory_space=pltpu.SMEM)
    dma = pltpu.SemaphoreType.DMA
    bf16, f32 = jnp.bfloat16, jnp.float32
    return pl.pallas_call(
        functools.partial(pair_kernel, n_row, n_col, n_sub),
        out_shape=jax.ShapeDtypeStruct((rows, half, width), bf16),
        in_specs=[smem] * 3 + [vmem] * 10,
        out_specs=vmem,
        scratch_shapes=[
            pltpu.VMEM((n_col, rows, cols, width), bf16),
            pltpu.VMEM((rows, total, 2 * width), bf16),
            pltpu.VMEM((rows, heads * half, width), bf16),
            pltpu.VMEM((rows, half, width), f32),
            pltpu.VMEM((rows, heads * half, total), f32),
            pltpu.VMEM((heads * half, total), f32),
            pltpu.VMEM((n_row, heads_here * rows, width), f32),
            pltpu.VMEM((owners, per_owner, heads_here * rows, width), f32),
            pltpu.VMEM((n_sub, 4, spread, width), bf16),
            pltpu.VMEM((n_sub, spread, width), bf16),
            pltpu.VMEM((rows, half, width), bf16),
            pltpu.VMEM((rows, half, width), f32),
            pltpu.VMEM((n_row, rows, half, width), bf16),
            pltpu.VMEM((rows, half, width), f32),
            pltpu.VMEM((2, rows * rows, width), f32),
            pltpu.VMEM((n_row, rows * rows, width), bf16),
            pltpu.VMEM((owners, per_owner, rows * rows, width), bf16),
            pltpu.VMEM((rows, half, width), f32),
            pltpu.VMEM((rows * half, width), f32),
            dma((2, 2)),
            dma((2, 2)),
            dma((4,)),
            dma((4,)),
            dma((2,)),
            dma((2,)),
            dma((n_row // STRIDE, len(LOCAL) + 2)),
            dma((n_row,)),
            dma((n_row,)),
            dma((owners, per_owner)),
            dma((2, 2, CHUNKS)),
            dma((2, n_row // 2, CHUNKS)),
            dma((n_row,)),
            dma((owners, per_owner)),
        ],
        compiler_params=pltpu.CompilerParams(collective_id=0, has_side_effects=True),
    )(
        length,
        chain,
        chain_bias,
        pair,
        chain,
        att_bias.T,
        att_proj.transpose(1, 2, 0),
        att_out,
        mult_in,
        mult_gate,
        mult_out,
        trans_up,
        trans_down,
    )


def solution(mesh):
    placed = (
        P(("grp", "row"), "col", None),
        P("grp"),
        P("grp"),
        P(None, None, "sub"),
        P(None, "sub"),
        P("sub"),
        P("sub", None),
        P(),
        P(),
        P(),
        P(),
        P(),
    )
    return jax.shard_map(
        local,
        mesh=mesh,
        in_specs=placed,
        out_specs=P(("grp", "row"), ("col", "sub"), None),
        check_vma=False,
    )
```

```python
import functools

import jax
import jax.numpy as jnp
from jax import lax
from jax.experimental import pallas as pl
from jax.experimental.pallas import tpu as pltpu
from jax.sharding import PartitionSpec as P

MESH = pl.DeviceIdType.MESH
CHUNKS = 4
STRIDE = 4
LOCAL = (-1, 1, 2)


def norm(value):
    mean = jnp.mean(value, axis=-1, keepdims=True)
    centred = value - mean
    variance = jnp.mean(centred * centred, axis=-1, keepdims=True)
    return centred * lax.rsqrt(variance + 1e-05)


def pair_kernel(
    n_row,
    n_col,
    n_sub,
    length_ref,
    chain_ref,
    chain_bias_ref,
    pair_ref,
    chain_lanes_ref,
    att_bias_ref,
    att_w_ref,
    att_out_ref,
    mult_in_ref,
    mult_gate_ref,
    mult_out_ref,
    trans_up_ref,
    trans_down_ref,
    out_ref,
    normed,
    kept,
    queries,
    att_gate,
    scores,
    bias,
    pieces,
    bias_in,
    both_w,
    both_out,
    attended,
    first_ref,
    gathered,
    left,
    stage_f32,
    stage,
    parts,
    tri,
    gate,
    x_send,
    x_recv,
    swap_send,
    swap_recv,
    weight_send,
    weight_recv,
    chain_send,
    chain_recv,
    bias_send,
    bias_recv,
    ring_send,
    ring_recv,
    part_send,
    part_recv,
):
    rows, cols, width = pair_ref.shape
    half = cols // n_sub
    total = rows * n_row
    piece = rows // CHUNKS
    block_rows = rows // 2
    heads_here = pieces.shape[1] // rows
    heads = heads_here * n_sub
    head_dim = width // heads
    z = lax.axis_index("row")
    x = lax.axis_index("col")
    core = lax.axis_index("sub")
    owners = n_col * n_sub
    me = x * n_sub + core
    per_owner = n_row // owners
    far = n_row // 2
    up = lax.rem(z + 1, n_row)
    down = lax.rem(z + n_row - 1, n_row)
    length = length_ref[0]

    def row_at(offset):
        return lax.rem(z + (offset + n_row), n_row)

    barrier = pltpu.get_barrier_semaphore()
    near = (1, -1, 2, -2, STRIDE, -STRIDE)
    for offset in near:
        pl.semaphore_signal(
            barrier, inc=1, device_id={"row": row_at(offset)}, device_id_type=MESH
        )
    for step in range(1, owners):
        other = lax.rem(me + step, owners)
        pl.semaphore_signal(
            barrier,
            inc=1,
            device_id={"col": lax.div(other, n_sub), "sub": lax.rem(other, n_sub)},
            device_id_type=MESH,
        )

    normed[x] = norm(pair_ref[...].astype(jnp.float32)).astype(jnp.bfloat16)
    both_out[core] = att_out_ref[...]
    both_w[core] = att_w_ref[...]

    lane = lax.broadcasted_iota(jnp.int32, (1, width), 1)
    begin = x * cols
    turn = lax.rem(begin, width)
    key = begin + lax.rem(lane + (width - turn), width)
    key_chain = jnp.zeros((1, width), jnp.int32)
    for k in range(total // width):
        held = chain_lanes_ref[k * width : (k + 1) * width].reshape(1, width)
        key_chain = jnp.where(key // width == k, held, key_chain)
    key_bias = ((key < length).astype(jnp.float32) - 1.0) * 1000000000.0
    padding = jnp.zeros((width - cols, width), jnp.bfloat16)
    bias_w = att_bias_ref[...]
    for i in range(rows):
        keys_i = jnp.concatenate([normed[x, i], padding], axis=0)
        term = lax.dot_general(
            bias_w, keys_i, (((1,), (1,)), ((), ())), preferred_element_type=jnp.float32
        )
        term = pltpu.roll(term, turn, 1)
        same = (key_chain == chain_ref[z * rows + i]).astype(jnp.float32)
        for h in range(heads_here):
            at = h * rows + i
            pieces[z, at : at + 1] = term[h : h + 1] + chain_bias_ref[h] * same + key_bias

    pl.semaphore_wait(barrier, len(near) + owners - 1)

    def weight_copy(k):
        source, target = [
            (att_w_ref, both_w.at[core]),
            (att_out_ref, both_out.at[core]),
        ][k]
        return pltpu.make_async_remote_copy(
            src_ref=source,
            dst_ref=target,
            send_sem=weight_send.at[k],
            recv_sem=weight_recv.at[k],
            device_id={"sub": 1 - core},
            device_id_type=MESH,
        )

    quarter = block_rows // 2
    x_up = lax.rem(x + n_col - 1, n_col)
    x_down = lax.rem(x + 1, n_col)
    x_far = lax.rem(x + 2, n_col)

    def x_copy(way, step, arrives):
        distance = step + 1 if arrives else step
        source = lax.rem(x + (n_col - distance if way == 0 else distance), n_col)
        begin_row = core * block_rows + (quarter if step == 1 and way == 1 else 0)
        block = normed.at[source, pl.ds(begin_row, block_rows if step == 0 else quarter)]
        return pltpu.make_async_remote_copy(
            src_ref=block,
            dst_ref=block,
            send_sem=x_send.at[way, step],
            recv_sem=x_recv.at[way, step],
            device_id={"col": lax.rem(x + (1 if way == 0 else n_col - 1), n_col)},
            device_id_type=MESH,
        )

    def swap(k, holder):
        source = (x_up, x_down, x_far, x_far)[k]
        begin_row = holder * block_rows + (quarter if k == 3 else 0)
        block = normed.at[source, pl.ds(begin_row, block_rows if k < 2 else quarter)]
        return pltpu.make_async_remote_copy(
            src_ref=block,
            dst_ref=block,
            send_sem=swap_send.at[k],
            recv_sem=swap_recv.at[k],
            device_id={"sub": 1 - core},
            device_id_type=MESH,
        )

    def bias_hop(stop, k, block, offset):
        return pltpu.make_async_remote_copy(
            src_ref=pieces.at[block],
            dst_ref=pieces.at[block],
            send_sem=chain_send.at[stop, k],
            recv_sem=chain_recv.at[block],
            device_id={"row": row_at(offset)},
            device_id_type=MESH,
        )

    def owner_copy(block, source, target, send_sem, recv_sem):
        dest = lax.div(block, per_owner)
        return pltpu.make_async_remote_copy(
            src_ref=source.at[block],
            dst_ref=target.at[me, lax.rem(block, per_owner)],
            send_sem=send_sem.at[block],
            recv_sem=recv_sem.at[me, lax.rem(block, per_owner)],
            device_id={"col": lax.div(dest, n_sub), "sub": lax.rem(dest, n_sub)},
            device_id_type=MESH,
        )

    def to_owner(block, source, target, send_sem, recv_sem):
        slot = lax.rem(block, per_owner)
        mine = lax.div(block, per_owner) == me

        @pl.when(mine)
        def _():
            pltpu.make_async_copy(
                source.at[block], target.at[me, slot], recv_sem.at[me, slot]
            ).start()

        @pl.when(jnp.logical_not(mine))
        def _():
            owner_copy(block, source, target, send_sem, recv_sem).start()

    bias_way = (pieces, bias_in, bias_send, bias_recv)
    part_way = (stage, parts, part_send, part_recv)
    ups = n_row // (2 * STRIDE)

    def hops_of(stop):
        if stop == 0:
            ahead = [(0, STRIDE), (len(LOCAL) + 1, -STRIDE)]
        elif stop < ups:
            ahead = [(0, STRIDE)]
        elif stop == ups or stop == 2 * ups - 1:
            ahead = []
        else:
            ahead = [(0, -STRIDE)]
        return ahead + [(1 + n, offset) for n, offset in enumerate(LOCAL)]

    def block_of(stop):
        return row_at(-STRIDE * stop if stop <= ups else STRIDE * (stop - ups))

    def pass_on(stop):
        block = block_of(stop)
        if stop > 0:
            bias_hop(stop, 0, block, 0).wait_recv()
        for k, offset in hops_of(stop):
            bias_hop(stop, k, block, offset).start()
        to_owner(block, *bias_way)

    def take_local(stop):
        for offset in LOCAL:
            block = lax.rem(block_of(stop) + (n_row - offset), n_row)
            bias_hop(stop, 0, block, 0).wait_recv()
            to_owner(block, *bias_way)

    def project(source, chunk):
        tile = normed[source, pl.ds(chunk * block_rows, block_rows)]
        made = times(tile.reshape(block_rows * cols, width), w_kept).astype(jnp.bfloat16)
        kept[
            pl.ds(chunk * block_rows, block_rows), pl.ds(pl.multiple_of(source * cols, 32), cols)
        ] = made.reshape(block_rows, cols, 2 * width)

    def score(i, carry):
        scores[i] = lax.dot_general(
            queries[i],
            kept[i, :, :width],
            (((1,), (1,)), ((), ())),
            preferred_element_type=jnp.float32,
        )
        return carry

    for way in range(2):
        x_copy(way, 0, False).start()
    pass_on(0)
    for k in range(2):
        weight_copy(k).start()
    for k in range(2):
        weight_copy(k).wait_recv()

    def joined(g):
        return jnp.concatenate([both_w[k, g] for k in range(n_sub)], axis=0)

    def times(value, weight):
        return lax.dot_general(
            value, weight, (((1,), (1,)), ((), ())), preferred_element_type=jnp.float32
        )

    w_query, w_gate = joined(0), joined(3)
    w_kept = jnp.concatenate([joined(1), joined(2)], axis=0)
    tile = normed[x, :, pl.ds(pl.multiple_of(core * half, 16), half)].reshape(rows * half, width)
    query = (times(tile, w_query) * head_dim ** (-0.5)).astype(jnp.bfloat16)
    head_of = lax.broadcasted_iota(jnp.int32, (rows * half, width), 1) // head_dim
    for h in range(heads):
        queries[:, h * half : (h + 1) * half] = jnp.where(
            head_of == h, query, jnp.zeros_like(query)
        ).reshape(rows, half, width)
    att_gate[...] = jax.nn.sigmoid(times(tile, w_gate)).reshape(rows, half, width)
    for chunk in range(2):
        project(x, chunk)

    def stage_of(step):
        take_local(step - 1)
        if step > 1:
            take_local(ups + step - 1)
        pass_on(step)
        if step < ups:
            pass_on(ups + step)

    for way in range(2):
        x_copy(way, 0, True).wait_recv()
        x_copy(way, 1, False).start()
        swap(way, core).start()
    stage_of(1)
    project(x_up, core)
    project(x_down, core)
    for way in range(2):
        x_copy(way, 1, True).wait_recv()
        swap(2 + way, core).start()
    stage_of(2)
    project(x_far, core)
    swap(0, 1 - core).wait_recv()
    project(x_up, 1 - core)
    swap(1, 1 - core).wait_recv()
    project(x_down, 1 - core)
    stage_of(3)
    swap(2, 1 - core).wait_recv()
    swap(3, 1 - core).wait_recv()
    project(x_far, 1 - core)
    lax.fori_loop(0, block_rows, score, 0)
    stage_of(4)
    lax.fori_loop(block_rows, rows, score, 0)
    take_local(ups)

    for slot in range(per_owner):
        for giver in range(owners):
            pltpu.make_async_copy(
                pieces.at[0], bias_in.at[giver, slot], bias_recv.at[giver, slot]
            ).wait()
    lane = lax.broadcasted_iota(jnp.int32, (rows, width), 1)
    for slot in range(per_owner):
        for h in range(heads):
            giver, own_head = h // heads_here, h % heads_here
            held = [
                bias_in[k * n_sub + giver, slot, own_head * rows : (own_head + 1) * rows]
                for k in range(n_col)
            ]
            at = h * half + slot * rows
            for k in range(total // width):
                line = None
                for source in range(n_col):
                    begin = source * cols - k * width
                    if begin + cols <= 0 or begin >= width:
                        continue
                    line = held[source] if line is None else jnp.where(lane >= begin, held[source], line)
                bias[at : at + rows, k * width : (k + 1) * width] = line

    head_of = lax.broadcasted_iota(jnp.int32, (half, width), 1) // head_dim

    def attend(i, carry):
        logits = scores[i] + bias[...]
        weights = jnp.exp(logits - jnp.max(logits, axis=-1, keepdims=True))
        weights = weights * (1.0 / jnp.sum(weights, axis=-1, keepdims=True))
        mixed_values = jnp.dot(
            weights.astype(jnp.bfloat16), kept[i, :, width:], preferred_element_type=jnp.float32
        )
        taken = jnp.zeros((half, width), jnp.float32)
        for h in range(heads):
            taken = jnp.where(head_of == h, mixed_values[h * half : (h + 1) * half], taken)
        attended[i] = (taken * att_gate[i]).astype(jnp.bfloat16)
        return carry

    lax.fori_loop(0, rows, attend, 0, unroll=2)
    first_ref[...] = pair_ref[:, pl.ds(pl.multiple_of(core * half, 16), half)].astype(
        jnp.float32
    ) + jnp.dot(
        attended[...].reshape(rows * half, width),
        both_out[...].reshape(width, width),
        preferred_element_type=jnp.float32,
    ).reshape(rows, half, width)

    first = first_ref[...].reshape(rows * half, width)
    mixed = norm(first).astype(jnp.bfloat16)
    quad = jnp.dot(mixed, mult_in_ref[...], preferred_element_type=jnp.float32)
    shape = (rows, half, width)
    here_row = z * rows + lax.broadcasted_iota(jnp.int32, shape, 0)
    here_col = (x * n_sub + core) * half + lax.broadcasted_iota(jnp.int32, shape, 1)
    valid = ((here_row < length) & (here_col < length)).astype(jnp.float32)
    a, b, c, d = [quad[:, k * width : (k + 1) * width].reshape(shape) for k in range(4)]
    left[...] = (valid * jax.nn.sigmoid(b) * a).astype(jnp.bfloat16).astype(jnp.float32)
    gathered[z] = (valid * jax.nn.sigmoid(d) * c).astype(jnp.bfloat16)
    gate[...] = jax.nn.sigmoid(
        jnp.dot(mixed, mult_gate_ref[...], preferred_element_type=jnp.float32)
    )

    def source(way, step):
        return lax.rem(z + (n_row - step if way == 0 else step), n_row)

    def ring_copy(way, step, chunk, arrives):
        block = gathered.at[source(way, step), pl.ds(chunk * piece, piece)]
        return pltpu.make_async_remote_copy(
            src_ref=block,
            dst_ref=block,
            send_sem=ring_send.at[way, lax.rem(step, 2), chunk],
            recv_sem=ring_recv.at[way, step - 1 if arrives else step, chunk],
            device_id={"row": up if way == 0 else down},
            device_id_type=MESH,
        )

    def hop(way, step, chunk):
        return ring_copy(way, step, chunk, False)

    def arrival(way, step, chunk):
        return ring_copy(way, step, chunk, True)

    def multiply(owner, chunk, lane):
        for jj in range(piece):
            j = chunk * piece + jj
            right = gathered[owner, j].astype(jnp.float32)
            for i in range(rows):
                stage_f32[lane, pl.ds(i * rows + j, 1)] = jnp.sum(
                    left[i] * right, axis=0, keepdims=True
                )

    def give(block, lane):
        stage[block] = stage_f32[lane].astype(jnp.bfloat16)
        to_owner(block, *part_way)

    for chunk in range(CHUNKS):
        for way in range(2):
            hop(way, 0, chunk).start()

    def own(chunk, carry):
        multiply(z, chunk, 0)
        return carry

    lax.fori_loop(0, CHUNKS, own, 0)
    give(z, 0)

    def visit(n, carry):
        step = lax.div(n, CHUNKS) + 1
        chunk = lax.rem(n, CHUNKS)
        for way in range(2):
            arrival(way, step, chunk).wait_recv()
            last = chunk < CHUNKS // 2 if way == 0 else chunk >= CHUNKS // 2

            @pl.when(step >= 2)
            def _():
                hop(way, step, chunk).wait_send()

            @pl.when(jnp.logical_or(step < far - 1, last))
            def _():
                hop(way, step, chunk).start()

        for way in range(2):
            multiply(source(way, step), chunk, way)

        @pl.when(chunk == CHUNKS - 1)
        def _():
            for way in range(2):
                give(source(way, step), way)

        return carry

    lax.fori_loop(0, (far - 1) * CHUNKS, visit, 0)

    for chunk in range(CHUNKS):
        arrival(0 if chunk < CHUNKS // 2 else 1, far, chunk).wait_recv()
        multiply(source(0, far), chunk, 0)
    give(source(0, far), 0)

    for way in range(2):
        for chunk in range(CHUNKS):
            hop(way, far - 2, chunk).wait_send()
            if (chunk < CHUNKS // 2) == (way == 0):
                hop(way, far - 1, chunk).wait_send()

    for stop in range(2 * ups):
        for k, offset in hops_of(stop):
            bias_hop(stop, k, block_of(stop), offset).wait_send()
    for k in range(2):
        weight_copy(k).wait_send()
    for way in range(2):
        for step in range(2):
            x_copy(way, step, False).wait_send()
    for k in range(4):
        swap(k, core).wait_send()

    def sent(block, carry):
        @pl.when(lax.div(block, per_owner) != me)
        def _():
            owner_copy(block, *bias_way).wait_send()
            owner_copy(block, *part_way).wait_send()

        return carry

    lax.fori_loop(0, n_row, sent, 0)

    for slot in range(per_owner):
        total_f32 = None
        for giver in range(owners):
            pltpu.make_async_copy(
                stage.at[0], parts.at[giver, slot], part_recv.at[giver, slot]
            ).wait()
            part = parts[giver, slot].astype(jnp.float32)
            total_f32 = part if total_f32 is None else total_f32 + part
        for i in range(rows):
            tri[i, slot * rows : (slot + 1) * rows] = total_f32[i * rows : (i + 1) * rows]

    tri_normed = norm(tri[...].reshape(rows * half, width)).astype(jnp.bfloat16)
    second = first_ref[...].reshape(rows * half, width) + gate[...] * jnp.dot(
        tri_normed, mult_out_ref[...], preferred_element_type=jnp.float32
    )
    last_normed = norm(second).astype(jnp.bfloat16)
    hidden = jax.nn.relu(
        jnp.dot(last_normed, trans_up_ref[...], preferred_element_type=jnp.float32)
    ).astype(jnp.bfloat16)
    result = second + jnp.dot(hidden, trans_down_ref[...], preferred_element_type=jnp.float32)
    out_ref[...] = result.astype(jnp.bfloat16).reshape(rows, half, width)


def local(
    pair,
    length,
    chain,
    att_proj,
    att_bias,
    chain_bias,
    att_out,
    mult_in,
    mult_gate,
    mult_out,
    trans_up,
    trans_down,
):
    rows, cols, width = pair.shape
    n_row, n_col, n_sub = (lax.axis_size(a) for a in ("row", "col", "sub"))
    owners = n_col * n_sub
    per_owner = n_row // owners
    half = cols // n_sub
    total = rows * n_row
    heads_here = att_bias.shape[1]
    heads = heads_here * n_sub
    spread = att_out.shape[0]
    vmem = pl.BlockSpec(memory_space=pltpu.VMEM)
    smem = pl.BlockSpec(memory_space=pltpu.SMEM)
    dma = pltpu.SemaphoreType.DMA
    bf16, f32 = jnp.bfloat16, jnp.float32
    return pl.pallas_call(
        functools.partial(pair_kernel, n_row, n_col, n_sub),
        out_shape=jax.ShapeDtypeStruct((rows, half, width), bf16),
        in_specs=[smem] * 3 + [vmem] * 10,
        out_specs=vmem,
        scratch_shapes=[
            pltpu.VMEM((n_col, rows, cols, width), bf16),
            pltpu.VMEM((rows, total, 2 * width), bf16),
            pltpu.VMEM((rows, heads * half, width), bf16),
            pltpu.VMEM((rows, half, width), f32),
            pltpu.VMEM((rows, heads * half, total), f32),
            pltpu.VMEM((heads * half, total), f32),
            pltpu.VMEM((n_row, heads_here * rows, width), f32),
            pltpu.VMEM((owners, per_owner, heads_here * rows, width), f32),
            pltpu.VMEM((n_sub, 4, spread, width), bf16),
            pltpu.VMEM((n_sub, spread, width), bf16),
            pltpu.VMEM((rows, half, width), bf16),
            pltpu.VMEM((rows, half, width), f32),
            pltpu.VMEM((n_row, rows, half, width), bf16),
            pltpu.VMEM((rows, half, width), f32),
            pltpu.VMEM((2, rows * rows, width), f32),
            pltpu.VMEM((n_row, rows * rows, width), bf16),
            pltpu.VMEM((owners, per_owner, rows * rows, width), bf16),
            pltpu.VMEM((rows, half, width), f32),
            pltpu.VMEM((rows * half, width), f32),
            dma((2, 2)),
            dma((2, 2)),
            dma((4,)),
            dma((4,)),
            dma((2,)),
            dma((2,)),
            dma((n_row // STRIDE, len(LOCAL) + 2)),
            dma((n_row,)),
            dma((n_row,)),
            dma((owners, per_owner)),
            dma((2, 2, CHUNKS)),
            dma((2, n_row // 2, CHUNKS)),
            dma((n_row,)),
            dma((owners, per_owner)),
        ],
        compiler_params=pltpu.CompilerParams(collective_id=0, has_side_effects=True),
    )(
        length,
        chain,
        chain_bias,
        pair,
        chain,
        att_bias.T,
        att_proj.transpose(1, 2, 0),
        att_out,
        mult_in,
        mult_gate,
        mult_out,
        trans_up,
        trans_down,
    )


def solution(mesh):
    placed = (
        P(("grp", "row"), "col", None),
        P("grp"),
        P("grp"),
        P(None, None, "sub"),
        P(None, "sub"),
        P("sub"),
        P("sub", None),
        P(),
        P(),
        P(),
        P(),
        P(),
    )
    return jax.shard_map(
        local,
        mesh=mesh,
        in_specs=placed,
        out_specs=P(("grp", "row"), ("col", "sub"), None),
        check_vma=False,
    )
```
